256 devices in a mesh: task: 32 (over x, z_hi, core), mp: 8 (over y, z_lo).
Axes of the slice: x: 4, y: 4, z: 8 (z_hi: 4, z_lo: 2; z = z_hi * 2 + z_lo), core: 2. Of those that a mesh axis runs over, the one named last changes fastest.
Arguments:
- hidden_in: bfloat16 [32768, 1024], P(('task', 'mp')), parts along dimension 0, may hold values from -16 to 16
- ff_gain: float32 [1024], replicated, may hold values from 0.5 to 1.5
- w_gate: bfloat16 [1024, 3072], P(None, 'mp'), may hold values from -0.1875 to 0.1875
- w_up: bfloat16 [1024, 3072], P(None, 'mp'), may hold values from -0.1875 to 0.1875
- w_out: bfloat16 [3072, 1024], P('mp'), may hold values from -0.109375 to 0.109375
- ff_rescale: float32 [98304], P(('task', 'mp')), parts along dimension 0, may hold values from 0.5 to 2
- final_gain: float32 [1024], replicated, may hold values from 0.5 to 1.5
- w_head: bfloat16 [1024, 16384], P(None, 'mp'), may hold values from -8 to 8
- targets: int32 [32768], P('task'), parts along dimension 0, may hold values from 0 to 16383
- lengths: int32 [128, 4], P('task'), parts along dimension 0, may hold values from 1 to 64, as said below
- labels: int32 [128], P('task'), parts along dimension 0, may hold values from 0 to 3
Outputs:
- scale_grad: float32 [98304], P(('task', 'mp')), parts along dimension 0
- loss_value: float32 [32], P('task'), parts along dimension 0
The draws below stay inside these ranges and needn't reach their ends.
There are 32 independent parts, one for each index of `task`. The reference program is written for one: setup_inputs(seed, part) draws one part's arguments, and reference() takes and returns one part's arrays. A program takes and returns all parts, laid end to end along the dimension named above; an argument that names none is the same for every part. Nothing has to cross between parts.
Inputs may be any that keep to these rules, and one draw needn't show every extreme that they name: `lengths`: every answer choice has at least one target token.
All inputs are finite; a program needn't handle non-finite values.
Results may differ from the reference program's by a relative error of at most 0.0067.
Values may be sent and summed in bfloat16 or wider, within the bound.
A program may use at most 64 MiB of HBM per device.

```python
import math
import jax
import jax.numpy as jnp
import numpy as np
from jax import lax

D = 1024
FF = 3072
V = 16384
CHOICES = 4
LEN = 64
EXAMPLES = 4
TOKENS = 1024


def draw_hidden_in(key, part):
    noise_key, first_key, second_key, third_key, level_key = jax.random.split(jax.random.fold_in(key, 11), 5)
    noise = jax.random.normal(noise_key, (TOKENS, D), jnp.float32)
    rows = jnp.arange(TOKENS, dtype=jnp.int32)
    first_row = jax.random.randint(first_key, (), 0, TOKENS)
    second_row = jax.random.randint(second_key, (), 0, TOKENS)
    third_row = jax.random.randint(third_key, (), 0, TOKENS)
    marked = (rows == first_row) | (rows == second_row) | (rows == third_row)
    level = jnp.exp(jax.random.uniform(level_key, (TOKENS,), jnp.float32, math.log(2.0), math.log(6.0)))
    shift = jnp.where(marked, level, 0.0)
    values = noise + shift[:, None]
    return jnp.clip(values, -16.0, 16.0).astype(jnp.bfloat16)


def draw_w_head(key, part):
    base_key, noise_key, column_key = jax.random.split(jax.random.fold_in(key, 23), 3)
    values = 3.0 * jax.random.normal(base_key, (D, V), jnp.float32) / math.sqrt(D)
    noise = jax.random.normal(noise_key, (D, V), jnp.float32)
    first = jax.random.randint(column_key, (), 0, V - 2)
    column = jnp.arange(V, dtype=jnp.int32)
    offset = (column - first).astype(jnp.float32)
    chosen = (column >= first) & (column < first + 3)
    factor = 1.0 - 0.007 * offset
    planted = 260.0 / D * factor[None, :] + 0.3 * noise / math.sqrt(D)
    values = jnp.where(chosen[None, :], planted, values)
    return jnp.clip(values, -8.0, 8.0).astype(jnp.bfloat16)


def draw_lengths(key, part):
    base_key, spot_key = jax.random.split(jax.random.fold_in(key, 37))
    total = EXAMPLES * CHOICES
    shortest = LEN - 3 * LEN // 8
    values = jax.random.randint(base_key, (total,), shortest, LEN + 1)
    spot = jax.random.randint(spot_key, (), 0, total)
    slots = jnp.arange(total, dtype=jnp.int32)
    values = jnp.where(slots == spot, 1, values)
    values = jnp.where(slots == (spot + 1) % total, LEN, values)
    return values.reshape(EXAMPLES, CHOICES).astype(jnp.int32)


def set_ends(array, key, least, largest):
    place = [jax.random.randint(jax.random.fold_in(key, axis), (), 0, length) for axis, length in enumerate(array.shape)]
    longest = array.shape.index(max(array.shape))
    next_to = place[:longest] + [(place[longest] + 1) % array.shape[longest]] + place[longest + 1:]
    return array.at[tuple(place)].set(least).at[tuple(next_to)].set(largest)


def block_scale(own_key, shape, shards, low, top_value):
    loudness = 1.0
    for dim, parts in shards:
        heights = jax.random.uniform(jax.random.fold_in(jax.random.fold_in(own_key, 6), dim), (parts,), jnp.float32, low / len(shards), top_value / len(shards))
        loudness = loudness * jnp.repeat(jnp.exp(heights), shape[dim] // parts).reshape((-1,) + (1,) * (len(shape) - 1 - dim))
    return loudness


def rank_bounds(number_of, skew):
    portions = [(1 << 20) // math.isqrt(standing ** skew) + 1 for standing in range(1, number_of + 1)]
    width = 1 + sum(portions) // (1 << 30)
    return np.cumsum(np.array([max(1, weight // width) for weight in portions]))


def ranked_ids(key, extent, number_of, skew):
    listing = rank_bounds(number_of, skew)
    ticket = jax.random.randint(jax.random.fold_in(key, 1), extent, 0, int(listing[number_of - 1]))
    grade = jnp.searchsorted(jnp.asarray(listing, jnp.int32), ticket, side="right")
    return jax.random.permutation(jax.random.fold_in(key, 2), number_of)[grade].astype(jnp.int32)


def scatter_about(key, extent, scale, bound, pieces=(), kind=jnp.bfloat16):
    level = block_scale(key, extent, pieces, -0.22, 0.18) if pieces else 1.0
    entries = jax.random.normal(key, extent, jnp.float32) * scale * level
    return jnp.minimum(jnp.maximum(entries, -bound), bound).astype(kind)


def setup_inputs(seed: int = 0, part: int = 0) -> dict:
    key_of = jax.random.split(jax.random.key(seed), 12)
    part_keys = jax.random.split(jax.random.fold_in(key_of[11], part), 12)
    return {
        "hidden_in": draw_hidden_in(jax.random.fold_in(jax.random.fold_in(key_of[11], part), 71), part),
        "ff_gain": jnp.clip(1.0 + 0.1 * jax.random.normal(key_of[1], (D,), jnp.float32), 0.5, 1.5),
        "w_gate": scatter_about(key_of[2], (D, FF), D ** -0.5, 0.1875, ((1, 8),)),
        "w_up": scatter_about(key_of[3], (D, FF), D ** -0.5, 0.1875, ((1, 8),)),
        "w_out": scatter_about(key_of[4], (FF, D), FF ** -0.5, 0.109375, ((0, 8),)),
        "ff_rescale": jnp.clip(jnp.exp(math.log(2.0) - 1.3862944 * jax.random.uniform(part_keys[5], (FF,), jnp.float32) ** block_scale(part_keys[5], (FF,), ((0, 8),), -0.2, 0.2)), 0.5, 2.0),
        "final_gain": jnp.clip(1.0 + 0.1 * jax.random.normal(key_of[6], (D,), jnp.float32), 0.5, 1.5),
        "w_head": draw_w_head(jax.random.fold_in(key_of[11], 71), part),
        "targets": set_ends(ranked_ids(part_keys[8], (TOKENS,), V, 2), jax.random.fold_in(part_keys[8], 3), 0, V - 1).astype(jnp.int32),
        "lengths": draw_lengths(jax.random.fold_in(jax.random.fold_in(key_of[11], part), 71), part),
        "labels": set_ends(jax.random.randint(part_keys[10], (EXAMPLES,), 0, CHOICES), jax.random.fold_in(part_keys[10], 1), 0, CHOICES - 1).astype(jnp.int32),
    }


epsilon = 1e-06

def rms_scale(values, gain):
    inverse = lax.rsqrt(lax.optimization_barrier(jnp.mean(values * values, axis=-1, keepdims=True)) + epsilon)
    return (values * inverse * gain, inverse)

def norm_back(values, inverse, gain, upstream):
    scaled = upstream * gain
    return inverse * scaled - values * inverse ** 3 * lax.optimization_barrier(jnp.mean(scaled * values, axis=-1, keepdims=True))

def task_loss(log_probs, lengths, labels):
    examples, choices = lengths.shape
    length = log_probs.shape[0] // (examples * choices)
    number_type = log_probs.dtype
    shaped = log_probs.reshape(examples, choices, length)
    position = jnp.arange(length, dtype=jnp.int32)
    valid = (position[None, None, :] < lengths[:, :, None]).astype(number_type)
    counts = lengths.astype(number_type)
    summed = lax.optimization_barrier(jnp.sum(shaped * valid, axis=-1))
    average = summed / counts
    correct = (jnp.arange(choices, dtype=jnp.int32)[None, :] == labels[:, None]).astype(number_type)
    wrong = 1.0 - correct
    likely = -jnp.sum(summed * correct) / jnp.sum(counts * correct)
    safe = jnp.where(valid > 0, shaped, -1.0)
    unlikely = -jnp.sum(jnp.log1p(-jnp.exp(safe)) * valid * wrong[:, :, None]) / jnp.sum(counts * wrong)
    normed = -jnp.mean(lax.optimization_barrier(jnp.sum(jax.nn.log_softmax(average, axis=-1) * correct, axis=-1)))
    return likely + unlikely + normed

def reference(hidden_in, ff_gain, w_gate, w_up, w_out, ff_rescale, final_gain, w_head, targets, lengths, labels):
    inputs = hidden_in.astype(jnp.float32)
    normed_in = rms_scale(inputs, ff_gain)[0].astype(jnp.bfloat16)
    gate_proj = jnp.dot(normed_in, w_gate, preferred_element_type=jnp.float32)
    up_proj = jnp.dot(normed_in, w_up, preferred_element_type=jnp.float32)
    activated = jax.nn.gelu(gate_proj, approximate=True) * up_proj
    hidden = (activated * ff_rescale).astype(jnp.bfloat16)
    residual = inputs + jnp.dot(hidden, w_out, preferred_element_type=jnp.float32)
    normed_out, inverse = rms_scale(residual, final_gain)
    logits = jnp.dot(normed_out.astype(jnp.bfloat16), w_head, preferred_element_type=jnp.float32)
    row_max = lax.optimization_barrier(jnp.max(logits, axis=1))
    row_sum = lax.optimization_barrier(jnp.sum(jnp.exp(logits - row_max[:, None]), axis=1))
    log_norm = row_max + jnp.log(row_sum)
    columns = jnp.arange(logits.shape[1], dtype=jnp.int32)[None, :]
    is_target = columns == targets[:, None]
    target_logit = lax.optimization_barrier(jnp.sum(jnp.where(is_target, logits, 0.0), axis=1))
    log_probs = target_logit - log_norm
    loss_value, pullback = jax.vjp(lambda values: task_loss(values, lengths, labels), log_probs)
    token_weight, = pullback(jnp.ones_like(loss_value))
    softmax_rows = jnp.exp(logits - log_norm[:, None])
    logit_grad = (token_weight[:, None] * (is_target.astype(logits.dtype) - softmax_rows)).astype(jnp.bfloat16)
    contract = (((1,), (1,)), ((), ()))
    normed_grad = lax.dot_general(logit_grad, w_head, contract, preferred_element_type=jnp.float32)
    resid_grad = norm_back(residual, inverse, final_gain, normed_grad).astype(jnp.bfloat16)
    hidden_grad = lax.dot_general(resid_grad, w_out, contract, preferred_element_type=jnp.float32)
    scale_grad = lax.optimization_barrier(jnp.sum(hidden_grad * activated, axis=0))
    return (scale_grad, loss_value.reshape(1))
```

```python
import functools
import math

import jax
import jax.numpy as jnp
from jax import lax
from jax.experimental import pallas as pl
from jax.experimental.pallas import tpu as pltpu
from jax.sharding import PartitionSpec as P

f32 = jnp.float32
bf16 = jnp.bfloat16
epsilon = 1e-06
ROOT = math.sqrt(2.0 / math.pi)
TILE = 512
STEPS = 256.0
TOP = 32700.0
WIDE = 1024 + 128

A, B = (0, 2), (2, 2)
AP, AM, BP, BM = (0, 1), (1, 1), (2, 1), (3, 1)


def coded(total):
    top = jnp.max(jnp.abs(total), axis=-1, keepdims=True)
    top = jnp.broadcast_to(jnp.maximum(top, 1e-30), (*total.shape[:-1], 128))
    power = jnp.ceil(jnp.log(top) * (STEPS / math.log(2.0)))
    factor = TOP * jnp.exp(power * (-math.log(2.0) / STEPS))
    value = jnp.round(total * jnp.concatenate([factor] * 8, axis=-1))
    both = jnp.concatenate([value, power], axis=-1)
    return both.astype(jnp.int32).astype(jnp.int16)


def decoded(code):
    both = code.astype(jnp.int32).astype(f32)
    factor = jnp.exp(both[..., 1024:] * (math.log(2.0) / STEPS)) * (1.0 / TOP)
    return both[..., :1024] * jnp.concatenate([factor] * 8, axis=-1)


class Links:
    def __init__(self, place, sends, recvs, log):
        y, z = place // 2, place % 2
        self.y, self.z = y, z
        self.yp, self.ym, self.yo = (y + 1) % 4, (y + 3) % 4, (y + 2) % 4
        self.oz = 1 - z
        self.to = {"z": y * 2 + (1 - z), "p": self.yp * 2 + z, "m": self.ym * 2 + z}
        self.sends, self.recvs, self.log = sends, recvs, log

    def copy(self, k, src, dst, way):
        return pltpu.make_async_remote_copy(
            src_ref=src,
            dst_ref=dst,
            send_sem=self.sends.at[k],
            recv_sem=self.recvs.at[k],
            device_id={"mp": self.to[way]},
            device_id_type=pl.DeviceIdType.MESH,
        )

    def send(self, k, src, dst, way):
        c = self.copy(k, src, dst, way)
        c.start()
        self.log.append(c)

    def got(self, k, dst):
        self.copy(k, dst, dst, "z").wait_recv()


class Gather(Links):
    def __init__(self, place, at, sends, recvs, log):
        super().__init__(place, sends, recvs, log)
        self.at = at

    def put(self, k, y, z, part, way):
        ref = self.at(y, z, part)
        self.send(k, ref, ref, way)

    def have(self, k, y, z, part):
        self.got(k, self.at(y, z, part))

    def s0(self):
        y, z = self.y, self.z
        self.put(0, y, z, A, "z")
        self.put(2, y, z, B, "p")
        self.put(3, y, z, B, "m")
        self.put(1, y, z, B, "z")
        self.put(4, y, z, A, "p")
        self.put(5, y, z, A, "m")

    def r1(self):
        self.have(2, self.ym, self.z, B)
        self.put(6, self.ym, self.z, BP, "p")
        self.put(15, self.ym, self.z, B, "z")
        self.have(3, self.yp, self.z, B)
        self.put(7, self.yp, self.z, BM, "m")
        self.put(14, self.yp, self.z, B, "z")

    def r2(self):
        self.have(0, self.y, self.oz, A)
        self.put(8, self.y, self.oz, A, "p")
        self.put(9, self.y, self.oz, A, "m")

    def r3(self):
        self.have(4, self.ym, self.z, A)
        self.put(10, self.ym, self.z, AP, "p")
        self.have(5, self.yp, self.z, A)
        self.put(11, self.yp, self.z, AM, "m")

    def r4(self):
        self.have(6, self.yo, self.z, BP)
        self.put(16, self.yo, self.z, BP, "z")
        self.have(7, self.yo, self.z, BM)
        self.put(17, self.yo, self.z, BM, "z")

    def r5(self):
        self.have(8, self.ym, self.oz, A)
        self.put(12, self.ym, self.oz, AP, "p")
        self.have(9, self.yp, self.oz, A)
        self.put(13, self.yp, self.oz, AM, "m")

    def own(self):
        self.have(1, self.y, self.oz, B)

    def plus(self):
        self.have(14, self.yp, self.oz, B)

    def minus(self):
        self.have(15, self.ym, self.oz, B)

    def far(self):
        self.have(10, self.yo, self.z, AP)
        self.have(11, self.yo, self.z, AM)
        self.have(12, self.yo, self.oz, AP)
        self.have(13, self.yo, self.oz, AM)
        self.have(16, self.yo, self.oz, BP)
        self.have(17, self.yo, self.oz, BM)


class Sum(Links):
    def __init__(self, place, g, part, out, halves, quarters, sends, recvs, log):
        super().__init__(place, sends, recvs, log)
        self.g, self.part, self.out, self.halves, self.quarters = g, part, out, halves, quarters

    def at(self, ref, y, z, part):
        return ref.at[self.g * 4 + y, z, pl.ds(*part)]

    def h(self, k):
        return self.halves.at[self.g, k]

    def q(self, k):
        return self.quarters.at[self.g, k]

    def s0_far(self):
        yo = self.yo
        for z in range(2):
            self.send(4 + 9 * z, self.at(self.out, yo, z, AP), self.q(0 + z), "p")
            self.send(5 + 9 * z, self.at(self.out, yo, z, AM), self.q(2 + z), "m")
        self.send(0, self.at(self.out, yo, self.oz, B), self.h(0), "z")

    def s0_plus(self):
        self.send(1, self.at(self.out, self.yp, self.oz, B), self.h(1), "z")

    def s0_minus(self):
        self.send(2, self.at(self.out, self.ym, self.oz, B), self.h(2), "z")

    def s0_own(self):
        self.send(3, self.at(self.out, self.y, self.oz, B), self.h(3), "z")

    def add(self, y, z, part, *refs):
        total = self.at(self.part, y, z, part)[...]
        for ref in refs:
            total = total + decoded(ref[...])
        self.at(self.out, y, z, part)[...] = coded(total)

    def s1(self):
        self.got(0, self.h(0))
        self.add(self.yo, self.z, B, self.h(0))
        self.send(8, self.at(self.out, self.yo, self.z, BP), self.q(4), "p")
        self.send(9, self.at(self.out, self.yo, self.z, BM), self.q(5), "m")
        for z in range(2):
            self.got(4 + 9 * z, self.q(0 + z))
            self.add(self.yp, z, AP, self.q(0 + z))
            self.send(6 + 9 * z, self.at(self.out, self.yp, z, A), self.h(4 + z), "p")
            self.got(5 + 9 * z, self.q(2 + z))
            self.add(self.ym, z, AM, self.q(2 + z))
            self.send(7 + 9 * z, self.at(self.out, self.ym, z, A), self.h(6 + z), "m")

    def s2(self):
        self.got(1, self.h(1))
        self.got(8, self.q(4))
        h = self.h(1)
        self.add(self.yp, self.z, BP, h.at[pl.ds(0, 1)], self.q(4))
        self.add(self.yp, self.z, BM, h.at[pl.ds(1, 1)])
        self.send(10, self.at(self.out, self.yp, self.z, B), self.h(8), "p")
        self.got(2, self.h(2))
        self.got(9, self.q(5))
        h = self.h(2)
        self.add(self.ym, self.z, BP, h.at[pl.ds(0, 1)])
        self.add(self.ym, self.z, BM, h.at[pl.ds(1, 1)], self.q(5))
        self.send(11, self.at(self.out, self.ym, self.z, B), self.h(9), "m")

    def s3(self):
        for z in range(2):
            self.got(6 + 9 * z, self.h(4 + z))
            self.got(7 + 9 * z, self.h(6 + z))
        self.add(self.y, self.oz, A, self.h(4 + self.oz), self.h(6 + self.oz))
        self.send(12, self.at(self.out, self.y, self.oz, A), self.h(10), "z")

    def result(self):
        self.got(3, self.h(3))
        self.got(10, self.h(8))
        self.got(11, self.h(9))
        self.got(12, self.h(10))
        halves = []
        for part, slots in ((A, (4 + self.z, 6 + self.z, 10)), (B, (3, 8, 9))):
            total = self.at(self.part, self.y, self.z, part)[...]
            for k in slots:
                total = total + decoded(self.h(k)[...])
            halves.append(total.reshape(32, 1024))
        return jnp.concatenate(halves, axis=0)


SUM_MESSAGES = 17
GATHER_MESSAGES = 18


def kernel(
    hidden_hbm,
    gate_hbm,
    up_hbm,
    out_hbm,
    head_hbm,
    ff_gain,
    final_gain,
    rescale,
    targets,
    lengths,
    labels,
    scale_grad,
    loss_out,
    x,
    w_in,
    w_out,
    w_out_t,
    w_head,
    w_head_t,
    act,
    tgt,
    part,
    out1,
    out2,
    halves1,
    quarters1,
    halves2,
    quarters2,
    normed,
    grads,
    logits,
    lgrad,
    res,
    stat,
    rows,
    acc,
    local_sem,
    g1_send,
    g1_recv,
    g2_send,
    g2_recv,
    s_send,
    s_recv,
    t_send,
    t_recv,
):
    place = lax.axis_index("mp")
    log = []
    own = pltpu.make_async_copy(hidden_hbm, x.at[place], local_sem.at[0])
    loads = [
        pltpu.make_async_copy(gate_hbm, w_in.at[:, pl.ds(0, 384)], local_sem.at[1]),
        pltpu.make_async_copy(up_hbm, w_in.at[:, pl.ds(384, 384)], local_sem.at[2]),
        pltpu.make_async_copy(out_hbm, w_out, local_sem.at[3]),
        pltpu.make_async_copy(head_hbm, w_head, local_sem.at[4]),
    ]
    own.start()
    for c in loads:
        c.start()

    barrier = pltpu.get_barrier_semaphore()
    for k in range(1, 8):
        pl.semaphore_signal(
            barrier,
            inc=1,
            device_id={"mp": (place + k) % 8},
            device_id_type=pl.DeviceIdType.MESH,
        )
    pl.semaphore_wait(barrier, 7)
    own.wait()

    first = Gather(
        place, lambda y, z, part: x.at[y * 2 + z, pl.ds(*part)], g1_send, g1_recv, log
    )
    first.s0()
    y, z, yp, ym, yo = first.y, first.z, first.yp, first.ym, first.yo

    def target_block(i, _):
        row = targets[pl.ds(i, 1), :].astype(f32)
        tgt[i] = jnp.transpose(jnp.broadcast_to(row, (128, 128)))
        return 0

    def head_block(i, _):
        r = pl.multiple_of((i // 8) * 256, 256)
        c = pl.multiple_of((i % 8) * 256, 256)
        w_head_t[pl.ds(c, 256), pl.ds(r, 256)] = jnp.transpose(
            w_head[pl.ds(r, 256), pl.ds(c, 256)]
        )
        return 0

    def out_block(i, _):
        r = pl.multiple_of((i // 4) * 128, 128)
        c = pl.multiple_of((i % 4) * 256, 256)
        w_out_t[pl.ds(c, 256), pl.ds(r, 128)] = jnp.transpose(
            w_out[pl.ds(r, 128), pl.ds(c, 256)]
        )
        return 0

    lax.fori_loop(0, 8, target_block, 0)
    acc[...] = jnp.zeros_like(acc)
    stat[...] = jnp.zeros_like(stat)
    loads[2].wait()
    lax.fori_loop(0, 12, out_block, 0)
    loads[3].wait()
    first.r1()
    first.r2()
    lax.fori_loop(0, 32, head_block, 0)
    first.r3()

    def feed_forward(e):
        rows2 = x[pl.ds(2 * e, 2)].reshape(256, 1024).astype(f32)
        inverse = lax.rsqrt(jnp.mean(rows2 * rows2, axis=-1, keepdims=True) + epsilon)
        n = (rows2 * inverse * ff_gain[...]).astype(bf16)
        both = jnp.dot(n, w_in[...], preferred_element_type=f32)
        gate, up = both[:, :384], both[:, 384:]
        cube = gate * gate * gate
        activated = gate * (0.5 * (1.0 + jnp.tanh(ROOT * (gate + 0.044715 * cube)))) * up
        act[pl.ds(2 * e, 2)] = activated.reshape(2, 128, 384)
        hidden = (activated * rescale[...]).astype(bf16)
        total = jnp.dot(hidden, w_out[...], preferred_element_type=f32)
        total = total.reshape(2, 2, 4, 16, 1024)
        part[pl.ds(2 * e, 2)] = total
        out1[pl.ds(2 * e, 2)] = coded(total)

    loads[0].wait()
    loads[1].wait()
    first.own()
    feed_forward(y)
    first.r4()
    first.r5()
    first.minus()
    feed_forward(ym)
    first.plus()
    feed_forward(yp)
    first.far()
    feed_forward(yo)

    sums = [
        Sum(place, g, part, out1, halves1, quarters1, s_send.at[g], s_recv.at[g], log)
        for g in range(2)
    ]
    for s in sums:
        s.s0_far()
        s.s0_plus()
        s.s0_minus()
        s.s0_own()
    for s in sums:
        s.s1()
    for s in sums:
        s.s2()
    for s in sums:
        s.s3()

    def gather_of(ref, sends, recvs, g):
        return Gather(
            place,
            lambda y, z, part: ref.at[g * 4 + y, z, pl.ds(*part)],
            sends.at[g],
            recvs.at[g],
            log,
        )

    nexts = [gather_of(normed, g2_send.at[0], g2_recv.at[0], g) for g in range(2)]
    lasts = [gather_of(grads, g2_send.at[1], g2_recv.at[1], g) for g in range(2)]

    def normed_rows(g):
        inputs = x[g * 4 + y, pl.ds(2 * z, 2)].reshape(64, 1024).astype(f32)
        residual = inputs + sums[g].result()
        res[g] = residual
        inverse = lax.rsqrt(jnp.mean(residual * residual, axis=-1, keepdims=True) + epsilon)
        n = (residual * inverse * final_gain[...]).astype(bf16)
        normed[g * 4 + y, z] = n.reshape(4, 16, 1024)

    lane = lax.broadcasted_iota(jnp.int32, (128, 128), 1)

    def logit_block(g, yy):
        b = g * 4 + yy
        n = normed[b].reshape(128, 1024)

        def tile(j, top):
            c = pl.multiple_of(j * TILE, TILE)
            value = jnp.dot(n, w_head[:, pl.ds(c, TILE)], preferred_element_type=f32)
            logits[b, :, pl.ds(c, TILE)] = value
            for k in range(TILE // 128):
                top = jnp.maximum(top, value[:, k * 128 : (k + 1) * 128])
            return top

        top = lax.fori_loop(0, 2048 // TILE, tile, jnp.full((128, 128), -jnp.inf, f32))
        top = jnp.max(top, axis=1, keepdims=True)
        wide = jnp.broadcast_to(top, (128, 128))
        wanted = tgt[b] - (place * 2048).astype(f32) - lane.astype(f32)

        def tally(j, so_far):
            total, hit = so_far
            for k in range(TILE // 128):
                c = pl.multiple_of(j * TILE + k * 128, 128)
                value = logits[b, :, pl.ds(c, 128)]
                total = total + jnp.exp(value - wide)
                hit = hit + jnp.where(wanted == c.astype(f32), value, 0.0)
            return total, hit

        zero = jnp.zeros((128, 128), f32)
        total, hit = lax.fori_loop(0, 2048 // TILE, tally, (zero, zero))
        total = jnp.sum(total, axis=1, keepdims=True)
        hit = jnp.sum(hit, axis=1, keepdims=True)
        table = jnp.where(lane == 0, top, jnp.where(lane == 1, total, hit))
        table = jnp.transpose(table)
        for k in range(3):
            stat[g, place, pl.ds(4 * k + yy, 1), :] = table[k : k + 1]

    def stat_copy(g, k):
        ref = stat.at[g, place]
        return pltpu.make_async_remote_copy(
            src_ref=ref,
            dst_ref=ref,
            send_sem=t_send.at[g, k - 1],
            recv_sem=t_recv.at[g, k - 1],
            device_id={"mp": (place + k) % 8},
            device_id_type=pl.DeviceIdType.MESH,
        )

    def send_stats(g):
        for k in range(1, 8):
            c = stat_copy(g, k)
            c.start()
            log.append(c)

    def wait_stats(g):
        for k in range(1, 8):
            ref = stat.at[g, (place + 8 - k) % 8]
            pltpu.make_async_remote_copy(
                src_ref=ref,
                dst_ref=ref,
                send_sem=t_send.at[g, k - 1],
                recv_sem=t_recv.at[g, k - 1],
                device_id={"mp": (place + k) % 8},
                device_id_type=pl.DeviceIdType.MESH,
            ).wait_recv()

    right = jnp.int32(0)
    whole = jnp.int32(0)
    for e in range(4):
        for c in range(4):
            right = right + jnp.where(labels[e] == c, lengths[e, c], 0)
            whole = whole + lengths[e, c]
    n_right = right.astype(f32)
    n_wrong = (whole - right).astype(f32)

    def loss_rows(g):
        top = stat[g, 0, 0:4]
        for k in range(1, 8):
            top = jnp.maximum(top, stat[g, k, 0:4])
        total = jnp.zeros((4, 128), f32)
        hit = jnp.zeros((4, 128), f32)
        for k in range(8):
            total = total + stat[g, k, 4:8] * jnp.exp(stat[g, k, 0:4] - top)
            hit = hit + stat[g, k, 8:12]
        log_norm = top + jnp.log(total)
        log_probs = hit - log_norm
        row = lax.broadcasted_iota(jnp.int32, (4, 128), 0)
        col = lax.broadcasted_iota(jnp.int32, (4, 128), 1)
        choice = (row % 2) * 2 + col // 64
        length = jnp.zeros((4, 128), jnp.int32)
        label = jnp.zeros((4, 128), jnp.int32)
        for i in range(4):
            e = g * 2 + i // 2
            label = jnp.where(row == i, labels[e], label)
            for s in range(2):
                here = (row == i) & (col // 64 == s)
                length = jnp.where(here, lengths[e, (i % 2) * 2 + s], length)
        valid = col % 64 < length
        correct = choice == label
        counts = length.astype(f32)
        kept = jnp.where(valid, log_probs, 0.0)
        low = jnp.sum(jnp.where(col < 64, kept, 0.0), axis=1, keepdims=True)
        high = jnp.sum(jnp.where(col < 64, 0.0, kept), axis=1, keepdims=True)
        average = jnp.where(col < 64, low, high) / counts
        safe = jnp.where(valid, log_probs, -1.0)
        prob = jnp.exp(safe)
        wrong = valid & ~correct
        likely = jnp.sum(jnp.where(correct, kept, 0.0))
        unlikely = jnp.sum(jnp.where(wrong, jnp.log1p(-prob), 0.0))
        normed_sum = jnp.float32(0.0)
        shares = []
        for i in range(2):
            a = average[2 * i : 2 * i + 2]
            shift = a - jnp.max(jnp.max(a, axis=1, keepdims=True), axis=0, keepdims=True)
            power = jnp.exp(shift)
            bulk = jnp.sum(jnp.sum(power, axis=1, keepdims=True), axis=0, keepdims=True)
            bulk = bulk * (1.0 / 64.0)
            shares.append(power / bulk)
            fine = jnp.where(correct[2 * i : 2 * i + 2], shift - jnp.log(bulk), 0.0)
            normed_sum = normed_sum + jnp.sum(fine) * (1.0 / 64.0)
        share = jnp.concatenate(shares, axis=0)
        weight = jnp.where(correct, -1.0 / n_right, prob / (1.0 - prob) / n_wrong)
        weight = weight - 0.25 * (jnp.where(correct, 1.0, 0.0) - share) / counts
        rows[g, 0:4] = log_norm
        rows[g, 4:8] = jnp.where(valid, weight, 0.0)
        return -likely / n_right - unlikely / n_wrong - 0.25 * normed_sum

    def grad_block(g, yy):
        b = g * 4 + yy
        norm_row = jnp.broadcast_to(rows[g, pl.ds(yy, 1), :], (128, 128))
        weight_row = jnp.broadcast_to(rows[g, pl.ds(4 + yy, 1), :], (128, 128))
        norm = jnp.transpose(norm_row)
        weight = jnp.transpose(weight_row)
        wanted = tgt[b] - (place * 2048).astype(f32) - lane.astype(f32)

        def tile(j, _):
            for k in range(TILE // 128):
                c = pl.multiple_of(j * TILE + k * 128, 128)
                soft = jnp.exp(logits[b, :, pl.ds(c, 128)] - norm)
                hot = jnp.where(wanted == c.astype(f32), 1.0, 0.0)
                lgrad[:, pl.ds(c, 128)] = (weight * (hot - soft)).astype(bf16)
            return 0

        lax.fori_loop(0, 2048 // TILE, tile, 0)

        def side(j, _):
            c = pl.multiple_of(j * TILE, TILE)
            value = jnp.dot(lgrad[...], w_head_t[:, pl.ds(c, TILE)], preferred_element_type=f32)
            value = value.reshape(2, 4, 16, TILE)
            part[b, :, :, :, pl.ds(c, TILE)] = value
            return 0

        lax.fori_loop(0, 1024 // TILE, side, 0)
        out2[b] = coded(part[b])

    normed_rows(0)
    nexts[0].s0()
    normed_rows(1)
    nexts[1].s0()
    nexts[0].r1()
    nexts[0].r2()
    nexts[1].r1()
    nexts[1].r2()
    nexts[0].r3()
    nexts[0].own()
    nexts[0].r4()
    nexts[0].r5()
    logit_block(0, y)
    nexts[1].r3()
    nexts[1].r4()
    nexts[0].minus()
    logit_block(0, ym)
    nexts[1].r5()
    nexts[0].plus()
    logit_block(0, yp)
    nexts[0].far()
    logit_block(0, yo)
    send_stats(0)
    nexts[1].own()
    logit_block(1, y)
    nexts[1].minus()
    logit_block(1, ym)
    wait_stats(0)
    loss = loss_rows(0)

    sums2 = [
        Sum(place, g, part, out2, halves2, quarters2, s_send.at[2 + g], s_recv.at[2 + g], log)
        for g in range(2)
    ]
    grad_block(0, yo)
    sums2[0].s0_far()
    grad_block(0, yp)
    sums2[0].s0_plus()
    grad_block(0, ym)
    sums2[0].s0_minus()
    grad_block(0, y)
    sums2[0].s0_own()
    nexts[1].plus()
    logit_block(1, yp)
    nexts[1].far()
    logit_block(1, yo)
    send_stats(1)
    sums2[0].s1()
    sums2[0].s2()
    wait_stats(1)
    loss = loss + loss_rows(1)
    loss_out[0] = loss
    grad_block(1, yo)
    sums2[1].s0_far()
    sums2[0].s3()
    grad_block(1, yp)
    sums2[1].s0_plus()
    grad_block(1, ym)
    sums2[1].s0_minus()
    grad_block(1, y)
    sums2[1].s0_own()

    def grad_rows(g):
        residual = res[g]
        inverse = lax.rsqrt(jnp.mean(residual * residual, axis=-1, keepdims=True) + epsilon)
        scaled = sums2[g].result() * final_gain[...]
        inner = jnp.mean(scaled * residual, axis=-1, keepdims=True)
        value = inverse * scaled - residual * (inverse * inverse * inverse) * inner
        grads[g * 4 + y, z] = value.astype(bf16).reshape(4, 16, 1024)

    def scale_block(g, yy):
        b = g * 4 + yy
        back = jnp.dot(grads[b].reshape(128, 1024), w_out_t[...], preferred_element_type=f32)
        acc[...] += jnp.sum((back * act[b]).reshape(16, 8, 384), axis=0)

    grad_rows(0)
    lasts[0].s0()
    sums2[1].s1()
    sums2[1].s2()
    lasts[0].r1()
    lasts[0].r2()
    sums2[1].s3()
    lasts[0].r3()
    lasts[0].r4()
    lasts[0].r5()
    grad_rows(1)
    lasts[1].s0()
    lasts[0].own()
    scale_block(0, y)
    lasts[1].r1()
    lasts[1].r2()
    lasts[0].minus()
    scale_block(0, ym)
    lasts[1].r3()
    lasts[0].plus()
    scale_block(0, yp)
    lasts[1].r4()
    lasts[1].r5()
    lasts[0].far()
    scale_block(0, yo)
    lasts[1].own()
    scale_block(1, y)
    lasts[1].minus()
    scale_block(1, ym)
    lasts[1].plus()
    scale_block(1, yp)
    lasts[1].far()
    scale_block(1, yo)
    scale_grad[...] = jnp.sum(acc[...], axis=0, keepdims=True)
    for c in log:
        c.wait_send()


def per_device(
    hidden_in, ff_gain, w_gate, w_up, w_out, ff_rescale, final_gain, w_head, targets, lengths, labels
):
    vmem = pl.BlockSpec(memory_space=pltpu.VMEM)
    smem = pl.BlockSpec(memory_space=pltpu.SMEM)
    hbm = pl.BlockSpec(memory_space=pl.ANY)
    dma = pltpu.SemaphoreType.DMA
    scale_grad, loss = pl.pallas_call(
        kernel,
        out_shape=(
            jax.ShapeDtypeStruct((1, 384), f32),
            jax.ShapeDtypeStruct((1,), f32),
        ),
        in_specs=[hbm] * 5 + [vmem] * 4 + [smem] * 2,
        out_specs=(vmem, smem),
        scratch_shapes=[
            pltpu.VMEM((8, 4, 32, 1024), bf16),
            pltpu.VMEM((1024, 768), bf16),
            pltpu.VMEM((384, 1024), bf16),
            pltpu.VMEM((1024, 384), bf16),
            pltpu.VMEM((1024, 2048), bf16),
            pltpu.VMEM((2048, 1024), bf16),
            pltpu.VMEM((8, 128, 384), f32),
            pltpu.VMEM((8, 128, 128), f32),
            pltpu.VMEM((8, 2, 4, 16, 1024), f32),
            pltpu.VMEM((8, 2, 4, 16, WIDE), jnp.int16),
            pltpu.VMEM((8, 2, 4, 16, WIDE), jnp.int16),
            pltpu.VMEM((2, 11, 2, 16, WIDE), jnp.int16),
            pltpu.VMEM((2, 6, 1, 16, WIDE), jnp.int16),
            pltpu.VMEM((2, 11, 2, 16, WIDE), jnp.int16),
            pltpu.VMEM((2, 6, 1, 16, WIDE), jnp.int16),
            pltpu.VMEM((8, 2, 4, 16, 1024), bf16),
            pltpu.VMEM((8, 2, 4, 16, 1024), bf16),
            pltpu.VMEM((8, 128, 2048), f32),
            pltpu.VMEM((128, 2048), bf16),
            pltpu.VMEM((2, 64, 1024), f32),
            pltpu.VMEM((2, 8, 16, 128), f32),
            pltpu.VMEM((2, 8, 128), f32),
            pltpu.VMEM((8, 384), f32),
            dma((5,)),
            dma((GATHER_MESSAGES,)),
            dma((GATHER_MESSAGES,)),
            dma((2, 2, GATHER_MESSAGES)),
            dma((2, 2, GATHER_MESSAGES)),
            dma((4, SUM_MESSAGES)),
            dma((4, SUM_MESSAGES)),
            dma((2, 7)),
            dma((2, 7)),
        ],
        compiler_params=pltpu.CompilerParams(
            collective_id=0, has_side_effects=True, vmem_limit_bytes=62 * 1024 * 1024
        ),
    )(
        hidden_in.reshape(4, 32, 1024),
        w_gate,
        w_up,
        w_out,
        w_head,
        ff_gain.reshape(1, 1024),
        final_gain.reshape(1, 1024),
        ff_rescale.reshape(1, 384),
        targets.reshape(8, 128),
        lengths,
        labels,
    )
    return (scale_grad.reshape(384), loss)


def solution(mesh):
    return jax.shard_map(
        per_device,
        mesh=mesh,
        in_specs=(
            P(("task", "mp"), None),
            P(),
            P(None, "mp"),
            P(None, "mp"),
            P("mp", None),
            P(("task", "mp")),
            P(),
            P(None, "mp"),
            P("task"),
            P("task", None),
            P("task"),
        ),
        out_specs=(P(("task", "mp")), P("task")),
        check_vma=False,
    )
```

```python
import functools
import math

import jax
import jax.numpy as jnp
from jax import lax
from jax.experimental import pallas as pl
from jax.experimental.pallas import tpu as pltpu
from jax.sharding import PartitionSpec as P

f32 = jnp.float32
bf16 = jnp.bfloat16
epsilon = 1e-06
ROOT = math.sqrt(2.0 / math.pi)
TILE = 512
HALF = 64
STEPS = 256.0
TOP = 32700.0
WIDE = 1024 + 128

A, B = (0, 2), (2, 2)
AP, AM, BP, BM = (0, 1), (1, 1), (2, 1), (3, 1)


def coded(total):
    top = jnp.max(jnp.abs(total), axis=-1, keepdims=True)
    top = jnp.broadcast_to(jnp.maximum(top, 1e-30), (*total.shape[:-1], 128))
    power = jnp.ceil(jnp.log(top) * (STEPS / math.log(2.0)))
    factor = TOP * jnp.exp(power * (-math.log(2.0) / STEPS))
    value = jnp.round(total * jnp.concatenate([factor] * 8, axis=-1))
    both = jnp.concatenate([value, power], axis=-1)
    return both.astype(jnp.int32).astype(jnp.int16)


def decoded(code):
    both = code.astype(jnp.int32).astype(f32)
    factor = jnp.exp(both[..., 1024:] * (math.log(2.0) / STEPS)) * (1.0 / TOP)
    return both[..., :1024] * jnp.concatenate([factor] * 8, axis=-1)


class Links:
    def __init__(self, place, sends, recvs, log):
        y, z = place // 2, place % 2
        self.y, self.z = y, z
        self.yp, self.ym, self.yo = (y + 1) % 4, (y + 3) % 4, (y + 2) % 4
        self.oz = 1 - z
        self.to = {"z": y * 2 + (1 - z), "p": self.yp * 2 + z, "m": self.ym * 2 + z}
        self.sends, self.recvs, self.log = sends, recvs, log

    def copy(self, k, src, dst, way):
        return pltpu.make_async_remote_copy(
            src_ref=src,
            dst_ref=dst,
            send_sem=self.sends.at[k],
            recv_sem=self.recvs.at[k],
            device_id={"mp": self.to[way]},
            device_id_type=pl.DeviceIdType.MESH,
        )

    def send(self, k, src, dst, way):
        c = self.copy(k, src, dst, way)
        c.start()
        self.log.append(c)

    def got(self, k, dst):
        self.copy(k, dst, dst, "z").wait_recv()


class Gather(Links):
    def __init__(self, place, at, sends, recvs, log):
        super().__init__(place, sends, recvs, log)
        self.at = at

    def put(self, k, y, z, part, way):
        ref = self.at(y, z, part)
        self.send(k, ref, ref, way)

    def have(self, k, y, z, part):
        self.got(k, self.at(y, z, part))

    def s0(self):
        y, z = self.y, self.z
        self.put(0, y, z, A, "z")
        self.put(2, y, z, B, "p")
        self.put(3, y, z, B, "m")
        self.put(1, y, z, B, "z")
        self.put(4, y, z, A, "p")
        self.put(5, y, z, A, "m")

    def r1(self):
        self.have(2, self.ym, self.z, B)
        self.put(6, self.ym, self.z, BP, "p")
        self.put(15, self.ym, self.z, B, "z")
        self.have(3, self.yp, self.z, B)
        self.put(7, self.yp, self.z, BM, "m")
        self.put(14, self.yp, self.z, B, "z")

    def r2(self):
        self.have(0, self.y, self.oz, A)
        self.put(8, self.y, self.oz, A, "p")
        self.put(9, self.y, self.oz, A, "m")

    def r3(self):
        self.have(4, self.ym, self.z, A)
        self.put(10, self.ym, self.z, AP, "p")
        self.have(5, self.yp, self.z, A)
        self.put(11, self.yp, self.z, AM, "m")

    def r4(self):
        self.have(6, self.yo, self.z, BP)
        self.put(16, self.yo, self.z, BP, "z")
        self.have(7, self.yo, self.z, BM)
        self.put(17, self.yo, self.z, BM, "z")

    def r5(self):
        self.have(8, self.ym, self.oz, A)
        self.put(12, self.ym, self.oz, AP, "p")
        self.have(9, self.yp, self.oz, A)
        self.put(13, self.yp, self.oz, AM, "m")

    def own(self):
        self.have(1, self.y, self.oz, B)

    def plus(self):
        self.have(14, self.yp, self.oz, B)

    def minus(self):
        self.have(15, self.ym, self.oz, B)

    def far(self):
        self.have(10, self.yo, self.z, AP)
        self.have(11, self.yo, self.z, AM)
        self.have(12, self.yo, self.oz, AP)
        self.have(13, self.yo, self.oz, AM)
        self.have(16, self.yo, self.oz, BP)
        self.have(17, self.yo, self.oz, BM)


class Sum(Links):
    def __init__(self, place, g, part, out, halves, quarters, sends, recvs, log):
        super().__init__(place, sends, recvs, log)
        self.g, self.part, self.out, self.halves, self.quarters = g, part, out, halves, quarters

    def at(self, ref, y, z, part):
        return ref.at[self.g * 4 + y, z, pl.ds(*part)]

    def h(self, k):
        return self.halves.at[self.g, k]

    def q(self, k):
        return self.quarters.at[self.g, k]

    def s0_far(self):
        yo = self.yo
        for z in range(2):
            self.send(4 + 9 * z, self.at(self.out, yo, z, AP), self.q(0 + z), "p")
            self.send(5 + 9 * z, self.at(self.out, yo, z, AM), self.q(2 + z), "m")
        self.send(0, self.at(self.out, yo, self.oz, B), self.h(0), "z")

    def s0_plus(self):
        self.send(1, self.at(self.out, self.yp, self.oz, B), self.h(1), "z")

    def s0_minus(self):
        self.send(2, self.at(self.out, self.ym, self.oz, B), self.h(2), "z")

    def s0_own(self):
        self.send(3, self.at(self.out, self.y, self.oz, B), self.h(3), "z")

    def add(self, y, z, part, *refs):
        total = self.at(self.part, y, z, part)[...]
        for ref in refs:
            total = total + decoded(ref[...])
        self.at(self.out, y, z, part)[...] = coded(total)

    def s1(self):
        self.got(0, self.h(0))
        self.add(self.yo, self.z, B, self.h(0))
        self.send(8, self.at(self.out, self.yo, self.z, BP), self.q(4), "p")
        self.send(9, self.at(self.out, self.yo, self.z, BM), self.q(5), "m")
        for z in range(2):
            self.got(4 + 9 * z, self.q(0 + z))
            self.add(self.yp, z, AP, self.q(0 + z))
            self.send(6 + 9 * z, self.at(self.out, self.yp, z, A), self.h(4 + z), "p")
            self.got(5 + 9 * z, self.q(2 + z))
            self.add(self.ym, z, AM, self.q(2 + z))
            self.send(7 + 9 * z, self.at(self.out, self.ym, z, A), self.h(6 + z), "m")

    def s2(self):
        self.got(1, self.h(1))
        self.got(8, self.q(4))
        h = self.h(1)
        self.add(self.yp, self.z, BP, h.at[pl.ds(0, 1)], self.q(4))
        self.add(self.yp, self.z, BM, h.at[pl.ds(1, 1)])
        self.send(10, self.at(self.out, self.yp, self.z, B), self.h(8), "p")
        self.got(2, self.h(2))
        self.got(9, self.q(5))
        h = self.h(2)
        self.add(self.ym, self.z, BP, h.at[pl.ds(0, 1)])
        self.add(self.ym, self.z, BM, h.at[pl.ds(1, 1)], self.q(5))
        self.send(11, self.at(self.out, self.ym, self.z, B), self.h(9), "m")

    def s3(self):
        for z in range(2):
            self.got(6 + 9 * z, self.h(4 + z))
            self.got(7 + 9 * z, self.h(6 + z))
        self.add(self.y, self.oz, A, self.h(4 + self.oz), self.h(6 + self.oz))
        self.send(12, self.at(self.out, self.y, self.oz, A), self.h(10), "z")

    def result(self):
        self.got(3, self.h(3))
        self.got(10, self.h(8))
        self.got(11, self.h(9))
        self.got(12, self.h(10))
        halves = []
        for part, slots in ((A, (4 + self.z, 6 + self.z, 10)), (B, (3, 8, 9))):
            total = self.at(self.part, self.y, self.z, part)[...]
            for k in slots:
                total = total + decoded(self.h(k)[...])
            halves.append(total.reshape(32, 1024))
        return jnp.concatenate(halves, axis=0)


SUM_MESSAGES = 17
GATHER_MESSAGES = 18


def kernel(
    hidden_hbm,
    gate_hbm,
    up_hbm,
    out_hbm,
    head_hbm,
    ff_gain,
    final_gain,
    rescale,
    targets,
    lengths,
    labels,
    scale_grad,
    loss_out,
    x,
    w_in,
    w_out,
    w_out_t,
    w_head,
    w_head_t,
    act,
    tgt,
    part,
    out1,
    out2,
    halves1,
    quarters1,
    halves2,
    quarters2,
    normed,
    grads,
    logits,
    lgrad,
    res,
    stat,
    rows,
    acc,
    local_sem,
    g1_send,
    g1_recv,
    g2_send,
    g2_recv,
    s_send,
    s_recv,
    t_send,
    t_recv,
):
    place = lax.axis_index("mp")
    log = []
    own = pltpu.make_async_copy(hidden_hbm, x.at[place], local_sem.at[0])
    loads = [
        pltpu.make_async_copy(gate_hbm, w_in.at[:, pl.ds(0, 384)], local_sem.at[1]),
        pltpu.make_async_copy(up_hbm, w_in.at[:, pl.ds(384, 384)], local_sem.at[2]),
        pltpu.make_async_copy(out_hbm, w_out, local_sem.at[3]),
        pltpu.make_async_copy(head_hbm, w_head, local_sem.at[4]),
    ]
    own.start()
    for c in loads:
        c.start()

    barrier = pltpu.get_barrier_semaphore()
    for k in range(1, 8):
        pl.semaphore_signal(
            barrier,
            inc=1,
            device_id={"mp": (place + k) % 8},
            device_id_type=pl.DeviceIdType.MESH,
        )
    pl.semaphore_wait(barrier, 7)
    own.wait()

    first = Gather(
        place, lambda y, z, part: x.at[y * 2 + z, pl.ds(*part)], g1_send, g1_recv, log
    )
    first.s0()
    y, z, yp, ym, yo = first.y, first.z, first.yp, first.ym, first.yo

    def target_block(i, _):
        row = targets[pl.ds(i, 1), :].astype(f32)
        tgt[i] = jnp.transpose(jnp.broadcast_to(row, (128, 128)))
        return 0

    def head_block(i, _):
        r = pl.multiple_of((i // 8) * 256, 256)
        c = pl.multiple_of((i % 8) * 256, 256)
        w_head_t[pl.ds(c, 256), pl.ds(r, 256)] = jnp.transpose(
            w_head[pl.ds(r, 256), pl.ds(c, 256)]
        )
        return 0

    def out_block(i, _):
        r = pl.multiple_of((i // 4) * 128, 128)
        c = pl.multiple_of((i % 4) * 256, 256)
        w_out_t[pl.ds(c, 256), pl.ds(r, 128)] = jnp.transpose(
            w_out[pl.ds(r, 128), pl.ds(c, 256)]
        )
        return 0

    lax.fori_loop(0, 8, target_block, 0)
    acc[...] = jnp.zeros_like(acc)
    stat[...] = jnp.zeros_like(stat)
    loads[2].wait()
    lax.fori_loop(0, 12, out_block, 0)
    loads[3].wait()
    first.r1()
    first.r2()
    lax.fori_loop(0, 32, head_block, 0)
    first.r3()

    def feed_forward(e):
        rows2 = x[pl.ds(2 * e, 2)].reshape(256, 1024).astype(f32)
        inverse = lax.rsqrt(jnp.mean(rows2 * rows2, axis=-1, keepdims=True) + epsilon)
        n = (rows2 * inverse * ff_gain[...]).astype(bf16)
        both = jnp.dot(n, w_in[...], preferred_element_type=f32)
        gate, up = both[:, :384], both[:, 384:]
        cube = gate * gate * gate
        activated = gate * (0.5 * (1.0 + jnp.tanh(ROOT * (gate + 0.044715 * cube)))) * up
        act[pl.ds(2 * e, 2)] = activated.reshape(2, 128, 384)
        hidden = (activated * rescale[...].reshape(1, 384)).astype(bf16)
        total = jnp.dot(hidden, w_out[...], preferred_element_type=f32)
        total = total.reshape(2, 2, 4, 16, 1024)
        part[pl.ds(2 * e, 2)] = total
        out1[pl.ds(2 * e, 2)] = coded(total)

    loads[0].wait()
    loads[1].wait()
    first.own()
    feed_forward(y)
    first.r4()
    first.r5()
    first.minus()
    feed_forward(ym)
    first.plus()
    feed_forward(yp)
    first.far()
    feed_forward(yo)

    sums = [
        Sum(place, g, part, out1, halves1, quarters1, s_send.at[g], s_recv.at[g], log)
        for g in range(2)
    ]
    for s in sums:
        s.s0_far()
        s.s0_plus()
        s.s0_minus()
        s.s0_own()
    for s in sums:
        s.s1()
    for s in sums:
        s.s2()
    for s in sums:
        s.s3()

    def gather_of(ref, sends, recvs, g):
        return Gather(
            place,
            lambda y, z, part: ref.at[g * 4 + y, z, pl.ds(*part)],
            sends.at[g],
            recvs.at[g],
            log,
        )

    nexts = [gather_of(normed, g2_send.at[0], g2_recv.at[0], g) for g in range(2)]
    lasts = [gather_of(grads, g2_send.at[1], g2_recv.at[1], g) for g in range(2)]

    def normed_rows(g):
        inputs = x[g * 4 + y, pl.ds(2 * z, 2)].reshape(64, 1024).astype(f32)
        residual = inputs + sums[g].result()
        res[g] = residual
        inverse = lax.rsqrt(jnp.mean(residual * residual, axis=-1, keepdims=True) + epsilon)
        n = (residual * inverse * final_gain[...]).astype(bf16)
        normed[g * 4 + y, z] = n.reshape(4, 16, 1024)

    lane = lax.broadcasted_iota(jnp.int32, (128, 128), 1)

    def wanted_of(b):
        return tgt[b] - (place * 2048).astype(f32) - lane.astype(f32)

    def logit_block(g, yy):
        b = g * 4 + yy
        n = normed[b].reshape(128, 1024)
        wanted = wanted_of(b)
        state = [
            (
                jnp.full((HALF, 128), -jnp.inf, f32),
                jnp.zeros((HALF, 128), f32),
                jnp.zeros((HALF, 128), f32),
            )
            for _ in range(128 // HALF)
        ]

        def tally(j):
            for i, (top, total, hit) in enumerate(state):
                r = slice(i * HALF, (i + 1) * HALF)
                starts = [j * TILE + k * 128 for k in range(TILE // 128)]
                values = [logits[b, r, c : c + 128] for c in starts]
                new = top
                for value in values:
                    new = jnp.maximum(new, value)
                total = total * jnp.exp(top - new)
                for c, value in zip(starts, values):
                    total = total + jnp.exp(value - new)
                    hit = hit + jnp.where(wanted[r] == c, value, 0.0)
                state[i] = (new, total, hit)

        tiles = 2048 // TILE
        for j in range(tiles):
            c = j * TILE
            logits[b, :, c : c + TILE] = jnp.dot(
                n, w_head[:, c : c + TILE], preferred_element_type=f32
            )
            if j:
                tally(j - 1)
        tally(tiles - 1)
        lanes, total, hit = (jnp.concatenate(v, axis=0) for v in zip(*state))
        top = jnp.max(lanes, axis=1, keepdims=True)
        total = jnp.sum(total * jnp.exp(lanes - top), axis=1, keepdims=True)
        hit = jnp.sum(hit, axis=1, keepdims=True)
        table = jnp.where(lane == 0, top, jnp.where(lane == 1, total, hit))
        table = jnp.transpose(table)
        for k in range(3):
            stat[g, place, pl.ds(4 * k + yy, 1), :] = table[k : k + 1]

    def stat_copy(g, k):
        ref = stat.at[g, place]
        return pltpu.make_async_remote_copy(
            src_ref=ref,
            dst_ref=ref,
            send_sem=t_send.at[g, k - 1],
            recv_sem=t_recv.at[g, k - 1],
            device_id={"mp": (place + k) % 8},
            device_id_type=pl.DeviceIdType.MESH,
        )

    def send_stats(g):
        for k in range(1, 8):
            c = stat_copy(g, k)
            c.start()
            log.append(c)

    def wait_stats(g):
        for k in range(1, 8):
            ref = stat.at[g, (place + 8 - k) % 8]
            pltpu.make_async_remote_copy(
                src_ref=ref,
                dst_ref=ref,
                send_sem=t_send.at[g, k - 1],
                recv_sem=t_recv.at[g, k - 1],
                device_id={"mp": (place + k) % 8},
                device_id_type=pl.DeviceIdType.MESH,
            ).wait_recv()

    right = jnp.int32(0)
    whole = jnp.int32(0)
    for e in range(4):
        for c in range(4):
            right = right + jnp.where(labels[e] == c, lengths[e, c], 0)
            whole = whole + lengths[e, c]
    n_right = right.astype(f32)
    n_wrong = (whole - right).astype(f32)

    def loss_rows(g):
        top = stat[g, 0, 0:4]
        for k in range(1, 8):
            top = jnp.maximum(top, stat[g, k, 0:4])
        total = jnp.zeros((4, 128), f32)
        hit = jnp.zeros((4, 128), f32)
        for k in range(8):
            total = total + stat[g, k, 4:8] * jnp.exp(stat[g, k, 0:4] - top)
            hit = hit + stat[g, k, 8:12]
        log_norm = top + jnp.log(total)
        log_probs = hit - log_norm
        row = lax.broadcasted_iota(jnp.int32, (4, 128), 0)
        col = lax.broadcasted_iota(jnp.int32, (4, 128), 1)
        choice = (row % 2) * 2 + col // 64
        length = jnp.zeros((4, 128), jnp.int32)
        label = jnp.zeros((4, 128), jnp.int32)
        for i in range(4):
            e = g * 2 + i // 2
            label = jnp.where(row == i, labels[e], label)
            for s in range(2):
                here = (row == i) & (col // 64 == s)
                length = jnp.where(here, lengths[e, (i % 2) * 2 + s], length)
        valid = col % 64 < length
        correct = choice == label
        counts = length.astype(f32)
        kept = jnp.where(valid, log_probs, 0.0)
        low = jnp.sum(jnp.where(col < 64, kept, 0.0), axis=1, keepdims=True)
        high = jnp.sum(jnp.where(col < 64, 0.0, kept), axis=1, keepdims=True)
        average = jnp.where(col < 64, low, high) / counts
        safe = jnp.where(valid, log_probs, -1.0)
        prob = jnp.exp(safe)
        wrong = valid & ~correct
        terms = jnp.where(correct, kept, 0.0) / n_right
        terms = terms + jnp.where(wrong, jnp.log1p(-prob), 0.0) / n_wrong
        fines = []
        shares = []
        for i in range(2):
            a = average[2 * i : 2 * i + 2]
            shift = a - jnp.max(jnp.max(a, axis=1, keepdims=True), axis=0, keepdims=True)
            power = jnp.exp(shift)
            bulk = jnp.sum(jnp.sum(power, axis=1, keepdims=True), axis=0, keepdims=True)
            bulk = bulk * (1.0 / 64.0)
            shares.append(power / bulk)
            fines.append(shift - jnp.log(bulk))
        share = jnp.concatenate(shares, axis=0)
        weight = jnp.where(correct, -1.0 / n_right, prob / (1.0 - prob) / n_wrong)
        weight = weight - 0.25 * (jnp.where(correct, 1.0, 0.0) - share) / counts
        rows[g, 0:4] = log_norm
        rows[g, 4:8] = jnp.where(valid, weight, 0.0)
        fine = jnp.where(correct, jnp.concatenate(fines, axis=0), 0.0)
        return -terms - fine * (0.25 / 64.0)

    def columns(row):
        return jnp.transpose(jnp.broadcast_to(row, (128, 128)))

    def softer(g, yy, slot):
        b = g * 4 + yy
        norm = columns(rows[g, pl.ds(yy, 1), :])
        weight = columns(rows[g, pl.ds(4 + yy, 1), :])
        wanted = wanted_of(b)

        def step(j):
            for k in range(TILE // 128):
                c = j * TILE + k * 128
                soft = jnp.exp(logits[b, :, c : c + 128] - norm)
                hot = jnp.where(wanted == c, 1.0, 0.0)
                lgrad[slot, :, c : c + 128] = (weight * (hot - soft)).astype(bf16)

        return step

    def grad_blocks(g, order, sends):
        step = softer(g, order[0], 0)
        for j in range(4):
            step(j)
        for i, yy in enumerate(order):
            b = g * 4 + yy
            step = softer(g, order[i + 1], (i + 1) % 2) if i + 1 < len(order) else None
            for j in range(4):
                value = jnp.dot(
                    lgrad[i % 2], w_head_t[:, j * 256 : (j + 1) * 256], preferred_element_type=f32
                )
                part[b, :, :, :, j * 256 : (j + 1) * 256] = value.reshape(2, 4, 16, 256)
                if step is not None:
                    step(j)
            out2[b] = coded(part[b])
            sends[i]()

    normed_rows(0)
    nexts[0].s0()
    normed_rows(1)
    nexts[1].s0()
    nexts[0].r1()
    nexts[0].r2()
    nexts[1].r1()
    nexts[1].r2()
    nexts[0].r3()
    nexts[0].own()
    nexts[0].r4()
    nexts[0].r5()
    logit_block(0, y)
    nexts[1].r3()
    nexts[1].r4()
    nexts[0].minus()
    logit_block(0, ym)
    nexts[1].r5()
    nexts[0].plus()
    logit_block(0, yp)
    nexts[0].far()
    logit_block(0, yo)
    send_stats(0)
    nexts[1].own()
    logit_block(1, y)
    nexts[1].minus()
    logit_block(1, ym)
    wait_stats(0)
    loss = loss_rows(0)

    sums2 = [
        Sum(place, g, part, out2, halves2, quarters2, s_send.at[2 + g], s_recv.at[2 + g], log)
        for g in range(2)
    ]
    s = sums2[0]
    grad_blocks(0, (yo, yp, ym, y), (s.s0_far, s.s0_plus, s.s0_minus, s.s0_own))
    nexts[1].plus()
    logit_block(1, yp)
    nexts[1].far()
    logit_block(1, yo)
    send_stats(1)
    sums2[0].s1()
    sums2[0].s2()
    wait_stats(1)
    loss = loss + loss_rows(1)
    sums2[0].s3()
    s = sums2[1]
    grad_blocks(1, (yo, yp, ym, y), (s.s0_far, s.s0_plus, s.s0_minus, s.s0_own))

    def grad_rows(g):
        residual = res[g]
        inverse = lax.rsqrt(jnp.mean(residual * residual, axis=-1, keepdims=True) + epsilon)
        scaled = sums2[g].result() * final_gain[...]
        inner = jnp.mean(scaled * residual, axis=-1, keepdims=True)
        value = inverse * scaled - residual * (inverse * inverse * inverse) * inner
        grads[g * 4 + y, z] = value.astype(bf16).reshape(4, 16, 1024)

    def scale_block(g, yy):
        b = g * 4 + yy
        back = jnp.dot(grads[b].reshape(128, 1024), w_out_t[...], preferred_element_type=f32)
        acc[...] += jnp.sum((back * act[b]).reshape(16, 8, 384), axis=0)

    grad_rows(0)
    lasts[0].s0()
    loss_out[0] = jnp.sum(loss)
    sums2[1].s1()
    sums2[1].s2()
    lasts[0].r1()
    lasts[0].r2()
    sums2[1].s3()
    lasts[0].r3()
    lasts[0].r4()
    lasts[0].r5()
    grad_rows(1)
    lasts[1].s0()
    lasts[0].own()
    scale_block(0, y)
    lasts[1].r1()
    lasts[1].r2()
    lasts[0].minus()
    scale_block(0, ym)
    lasts[1].r3()
    lasts[0].plus()
    scale_block(0, yp)
    lasts[1].r4()
    lasts[1].r5()
    lasts[0].far()
    scale_block(0, yo)
    lasts[1].own()
    scale_block(1, y)
    lasts[1].minus()
    scale_block(1, ym)
    lasts[1].plus()
    scale_block(1, yp)
    lasts[1].far()
    scale_block(1, yo)
    scale_grad[...] = jnp.sum(acc[...], axis=0)
    for c in log:
        c.wait_send()


def per_device(
    hidden_in, ff_gain, w_gate, w_up, w_out, ff_rescale, final_gain, w_head, targets, lengths, labels
):
    vmem = pl.BlockSpec(memory_space=pltpu.VMEM)
    smem = pl.BlockSpec(memory_space=pltpu.SMEM)
    hbm = pl.BlockSpec(memory_space=pl.ANY)
    dma = pltpu.SemaphoreType.DMA
    scale_grad, loss = pl.pallas_call(
        kernel,
        out_shape=(
            jax.ShapeDtypeStruct((384,), f32),
            jax.ShapeDtypeStruct((1,), f32),
        ),
        in_specs=[hbm] * 5 + [vmem] * 4 + [smem] * 2,
        out_specs=(vmem, smem),
        scratch_shapes=[
            pltpu.VMEM((8, 4, 32, 1024), bf16),
            pltpu.VMEM((1024, 768), bf16),
            pltpu.VMEM((384, 1024), bf16),
            pltpu.VMEM((1024, 384), bf16),
            pltpu.VMEM((1024, 2048), bf16),
            pltpu.VMEM((2048, 1024), bf16),
            pltpu.VMEM((8, 128, 384), f32),
            pltpu.VMEM((8, 128, 128), f32),
            pltpu.VMEM((8, 2, 4, 16, 1024), f32),
            pltpu.VMEM((8, 2, 4, 16, WIDE), jnp.int16),
            pltpu.VMEM((8, 2, 4, 16, WIDE), jnp.int16),
            pltpu.VMEM((2, 11, 2, 16, WIDE), jnp.int16),
            pltpu.VMEM((2, 6, 1, 16, WIDE), jnp.int16),
            pltpu.VMEM((2, 11, 2, 16, WIDE), jnp.int16),
            pltpu.VMEM((2, 6, 1, 16, WIDE), jnp.int16),
            pltpu.VMEM((8, 2, 4, 16, 1024), bf16),
            pltpu.VMEM((8, 2, 4, 16, 1024), bf16),
            pltpu.VMEM((8, 128, 2048), f32),
            pltpu.VMEM((2, 128, 2048), bf16),
            pltpu.VMEM((2, 64, 1024), f32),
            pltpu.VMEM((2, 8, 16, 128), f32),
            pltpu.VMEM((2, 8, 128), f32),
            pltpu.VMEM((8, 384), f32),
            dma((5,)),
            dma((GATHER_MESSAGES,)),
            dma((GATHER_MESSAGES,)),
            dma((2, 2, GATHER_MESSAGES)),
            dma((2, 2, GATHER_MESSAGES)),
            dma((4, SUM_MESSAGES)),
            dma((4, SUM_MESSAGES)),
            dma((2, 7)),
            dma((2, 7)),
        ],
        compiler_params=pltpu.CompilerParams(
            collective_id=0, has_side_effects=True, vmem_limit_bytes=62 * 1024 * 1024
        ),
    )(
        hidden_in.reshape(4, 32, 1024),
        w_gate,
        w_up,
        w_out,
        w_head,
        ff_gain.reshape(1, 1024),
        final_gain.reshape(1, 1024),
        ff_rescale,
        targets.reshape(8, 128),
        lengths,
        labels,
    )
    return (scale_grad, loss)


def solution(mesh):
    return jax.shard_map(
        per_device,
        mesh=mesh,
        in_specs=(
            P(("task", "mp"), None),
            P(),
            P(None, "mp"),
            P(None, "mp"),
            P("mp", None),
            P(("task", "mp")),
            P(),
            P(None, "mp"),
            P("task"),
            P("task", None),
            P("task"),
        ),
        out_specs=(P(("task", "mp")), P("task")),
        check_vma=False,
    )
```

```python
import functools
import math

import jax
import jax.numpy as jnp
from jax import lax
from jax.experimental import pallas as pl
from jax.experimental.pallas import tpu as pltpu
from jax.sharding import PartitionSpec as P

f32 = jnp.float32
bf16 = jnp.bfloat16
epsilon = 1e-06
ROOT = math.sqrt(2.0 / math.pi)
TILE = 512
HALF = 64
STEPS = 256.0
TOP = 32700.0
WIDE = 1024 + 128

A, B = (0, 2), (2, 2)
AP, AM, BP, BM = (0, 1), (1, 1), (2, 1), (3, 1)


def coded(total):
    top = jnp.max(jnp.abs(total), axis=-1, keepdims=True)
    top = jnp.broadcast_to(jnp.maximum(top, 1e-30), (*total.shape[:-1], 128))
    power = jnp.ceil(jnp.log(top) * (STEPS / math.log(2.0)))
    factor = TOP * jnp.exp(power * (-math.log(2.0) / STEPS))
    value = jnp.round(total * jnp.concatenate([factor] * 8, axis=-1))
    both = jnp.concatenate([value, power], axis=-1)
    return both.astype(jnp.int32).astype(jnp.int16)


def decoded(code):
    both = code.astype(jnp.int32).astype(f32)
    factor = jnp.exp(both[..., 1024:] * (math.log(2.0) / STEPS)) * (1.0 / TOP)
    return both[..., :1024] * jnp.concatenate([factor] * 8, axis=-1)


class Links:
    def __init__(self, place, sends, recvs, log):
        y, z = place // 2, place % 2
        self.y, self.z = y, z
        self.yp, self.ym, self.yo = (y + 1) % 4, (y + 3) % 4, (y + 2) % 4
        self.oz = 1 - z
        self.to = {"z": y * 2 + (1 - z), "p": self.yp * 2 + z, "m": self.ym * 2 + z}
        self.sends, self.recvs, self.log = sends, recvs, log

    def copy(self, k, src, dst, way):
        return pltpu.make_async_remote_copy(
            src_ref=src,
            dst_ref=dst,
            send_sem=self.sends.at[k],
            recv_sem=self.recvs.at[k],
            device_id={"mp": self.to[way]},
            device_id_type=pl.DeviceIdType.MESH,
        )

    def send(self, k, src, dst, way):
        c = self.copy(k, src, dst, way)
        c.start()
        self.log.append(c)

    def got(self, k, dst):
        self.copy(k, dst, dst, "z").wait_recv()


class Gather(Links):
    def __init__(self, place, at, sends, recvs, log):
        super().__init__(place, sends, recvs, log)
        self.at = at

    def put(self, k, y, z, part, way):
        ref = self.at(y, z, part)
        self.send(k, ref, ref, way)

    def have(self, k, y, z, part):
        self.got(k, self.at(y, z, part))

    def s0(self):
        y, z = self.y, self.z
        self.put(0, y, z, A, "z")
        self.put(2, y, z, B, "p")
        self.put(3, y, z, B, "m")
        self.put(1, y, z, B, "z")
        self.put(4, y, z, A, "p")
        self.put(5, y, z, A, "m")

    def r1(self):
        self.have(2, self.ym, self.z, B)
        self.put(6, self.ym, self.z, BP, "p")
        self.put(15, self.ym, self.z, B, "z")
        self.have(3, self.yp, self.z, B)
        self.put(7, self.yp, self.z, BM, "m")
        self.put(14, self.yp, self.z, B, "z")

    def r2(self):
        self.have(0, self.y, self.oz, A)
        self.put(8, self.y, self.oz, A, "p")
        self.put(9, self.y, self.oz, A, "m")

    def r3(self):
        self.have(4, self.ym, self.z, A)
        self.put(10, self.ym, self.z, AP, "p")
        self.have(5, self.yp, self.z, A)
        self.put(11, self.yp, self.z, AM, "m")

    def r4(self):
        self.have(6, self.yo, self.z, BP)
        self.put(16, self.yo, self.z, BP, "z")
        self.have(7, self.yo, self.z, BM)
        self.put(17, self.yo, self.z, BM, "z")

    def r5(self):
        self.have(8, self.ym, self.oz, A)
        self.put(12, self.ym, self.oz, AP, "p")
        self.have(9, self.yp, self.oz, A)
        self.put(13, self.yp, self.oz, AM, "m")

    def own(self):
        self.have(1, self.y, self.oz, B)

    def plus(self):
        self.have(14, self.yp, self.oz, B)

    def minus(self):
        self.have(15, self.ym, self.oz, B)

    def far(self):
        self.have(10, self.yo, self.z, AP)
        self.have(11, self.yo, self.z, AM)
        self.have(12, self.yo, self.oz, AP)
        self.have(13, self.yo, self.oz, AM)
        self.have(16, self.yo, self.oz, BP)
        self.have(17, self.yo, self.oz, BM)


class Sum(Links):
    def __init__(self, place, g, part, out, halves, quarters, sends, recvs, log):
        super().__init__(place, sends, recvs, log)
        self.g, self.part, self.out, self.halves, self.quarters = g, part, out, halves, quarters

    def at(self, ref, y, z, part):
        return ref.at[self.g * 4 + y, z, pl.ds(*part)]

    def h(self, k):
        return self.halves.at[self.g, k]

    def q(self, k):
        return self.quarters.at[self.g, k]

    def s0_far_y(self):
        yo = self.yo
        for z in range(2):
            self.send(4 + 9 * z, self.at(self.out, yo, z, AP), self.q(0 + z), "p")
            self.send(5 + 9 * z, self.at(self.out, yo, z, AM), self.q(2 + z), "m")

    def s0_far_z(self):
        self.send(0, self.at(self.out, self.yo, self.oz, B), self.h(0), "z")

    def s0_far(self):
        self.s0_far_y()
        self.s0_far_z()

    def s0_plus(self):
        self.send(1, self.at(self.out, self.yp, self.oz, B), self.h(1), "z")

    def s0_minus(self):
        self.send(2, self.at(self.out, self.ym, self.oz, B), self.h(2), "z")

    def s0_own(self):
        self.send(3, self.at(self.out, self.y, self.oz, B), self.h(3), "z")

    def add(self, y, z, part, *refs):
        total = self.at(self.part, y, z, part)[...]
        for ref in refs:
            total = total + decoded(ref[...])
        self.at(self.out, y, z, part)[...] = coded(total)

    def s1b(self):
        self.got(0, self.h(0))
        self.add(self.yo, self.z, B, self.h(0))
        self.send(8, self.at(self.out, self.yo, self.z, BP), self.q(4), "p")
        self.send(9, self.at(self.out, self.yo, self.z, BM), self.q(5), "m")

    def s1(self):
        self.s1b()
        self.s1a()

    def s1a(self):
        for z in range(2):
            self.got(4 + 9 * z, self.q(0 + z))
            self.add(self.yp, z, AP, self.q(0 + z))
            self.send(6 + 9 * z, self.at(self.out, self.yp, z, A), self.h(4 + z), "p")
            self.got(5 + 9 * z, self.q(2 + z))
            self.add(self.ym, z, AM, self.q(2 + z))
            self.send(7 + 9 * z, self.at(self.out, self.ym, z, A), self.h(6 + z), "m")

    def s2(self):
        self.got(1, self.h(1))
        self.got(8, self.q(4))
        h = self.h(1)
        self.add(self.yp, self.z, BP, h.at[pl.ds(0, 1)], self.q(4))
        self.add(self.yp, self.z, BM, h.at[pl.ds(1, 1)])
        self.send(10, self.at(self.out, self.yp, self.z, B), self.h(8), "p")
        self.got(2, self.h(2))
        self.got(9, self.q(5))
        h = self.h(2)
        self.add(self.ym, self.z, BP, h.at[pl.ds(0, 1)])
        self.add(self.ym, self.z, BM, h.at[pl.ds(1, 1)], self.q(5))
        self.send(11, self.at(self.out, self.ym, self.z, B), self.h(9), "m")

    def s3(self):
        for z in range(2):
            self.got(6 + 9 * z, self.h(4 + z))
            self.got(7 + 9 * z, self.h(6 + z))
        self.add(self.y, self.oz, A, self.h(4 + self.oz), self.h(6 + self.oz))
        self.send(12, self.at(self.out, self.y, self.oz, A), self.h(10), "z")

    def result(self):
        self.got(3, self.h(3))
        self.got(10, self.h(8))
        self.got(11, self.h(9))
        self.got(12, self.h(10))
        halves = []
        for part, slots in ((A, (4 + self.z, 6 + self.z, 10)), (B, (3, 8, 9))):
            total = self.at(self.part, self.y, self.z, part)[...]
            for k in slots:
                total = total + decoded(self.h(k)[...])
            halves.append(total.reshape(32, 1024))
        return jnp.concatenate(halves, axis=0)


SUM_MESSAGES = 17
GATHER_MESSAGES = 18


def kernel(
    hidden_hbm,
    gate_hbm,
    up_hbm,
    out_hbm,
    head_hbm,
    ff_gain_hbm,
    final_gain_hbm,
    rescale_hbm,
    targets_hbm,
    lengths_hbm,
    labels_hbm,
    scale_grad,
    loss_out,
    x,
    w_in,
    w_out,
    w_out_t,
    w_head,
    w_head_t,
    act,
    tgt,
    part,
    out1,
    out2,
    halves1,
    quarters1,
    halves2,
    quarters2,
    normed,
    grads,
    logits,
    lgrad,
    res,
    stat,
    rows,
    acc,
    ff_gain,
    final_gain,
    rescale,
    targets,
    lengths,
    labels,
    local_sem,
    g1_send,
    g1_recv,
    g2_send,
    g2_recv,
    s_send,
    s_recv,
    t_send,
    t_recv,
):
    place = lax.axis_index("mp")
    log = []
    own = pltpu.make_async_copy(hidden_hbm, x.at[place], local_sem.at[0])
    loads = [
        pltpu.make_async_copy(gate_hbm, w_in.at[:, pl.ds(0, 384)], local_sem.at[1]),
        pltpu.make_async_copy(up_hbm, w_in.at[:, pl.ds(384, 384)], local_sem.at[2]),
        pltpu.make_async_copy(out_hbm, w_out, local_sem.at[3]),
        pltpu.make_async_copy(head_hbm, w_head, local_sem.at[4]),
    ]
    small = [
        pltpu.make_async_copy(src, dst, local_sem.at[5 + k])
        for k, (src, dst) in enumerate(
            (
                (targets_hbm, targets),
                (ff_gain_hbm, ff_gain),
                (rescale_hbm, rescale),
                (final_gain_hbm, final_gain),
                (lengths_hbm, lengths),
                (labels_hbm, labels),
            )
        )
    ]
    own.start()
    for c in (*small, *loads):
        c.start()

    barrier = pltpu.get_barrier_semaphore()
    for k in range(1, 8):
        pl.semaphore_signal(
            barrier,
            inc=1,
            device_id={"mp": (place + k) % 8},
            device_id_type=pl.DeviceIdType.MESH,
        )
    pl.semaphore_wait(barrier, 7)
    own.wait()

    first = Gather(
        place, lambda y, z, part: x.at[y * 2 + z, pl.ds(*part)], g1_send, g1_recv, log
    )
    first.s0()
    y, z, yp, ym, yo = first.y, first.z, first.yp, first.ym, first.yo

    def target_block(i, _):
        row = targets[pl.ds(i, 1), :].astype(f32)
        tgt[i] = jnp.transpose(jnp.broadcast_to(row, (128, 128)))
        return 0

    def head_block(i, _):
        r = pl.multiple_of((i // 8) * 256, 256)
        c = pl.multiple_of((i % 8) * 256, 256)
        w_head_t[pl.ds(c, 256), pl.ds(r, 256)] = jnp.transpose(
            w_head[pl.ds(r, 256), pl.ds(c, 256)]
        )
        return 0

    def out_block(i, _):
        r = pl.multiple_of((i // 4) * 128, 128)
        c = pl.multiple_of((i % 4) * 256, 256)
        w_out_t[pl.ds(c, 256), pl.ds(r, 128)] = jnp.transpose(
            w_out[pl.ds(r, 128), pl.ds(c, 256)]
        )
        return 0

    for c in small:
        c.wait()
    lax.fori_loop(0, 8, target_block, 0)
    acc[...] = jnp.zeros_like(acc)
    stat[...] = jnp.zeros_like(stat)
    loads[2].wait()
    lax.fori_loop(0, 12, out_block, 0)
    loads[3].wait()
    first.r1()
    first.r2()
    lax.fori_loop(0, 32, head_block, 0)
    first.r3()

    def feed_forward(e):
        rows2 = x[pl.ds(2 * e, 2)].reshape(256, 1024).astype(f32)
        inverse = lax.rsqrt(jnp.mean(rows2 * rows2, axis=-1, keepdims=True) + epsilon)
        n = (rows2 * inverse * ff_gain[...]).astype(bf16)
        both = jnp.dot(n, w_in[...], preferred_element_type=f32)
        gate, up = both[:, :384], both[:, 384:]
        cube = gate * gate * gate
        activated = gate * (0.5 * (1.0 + jnp.tanh(ROOT * (gate + 0.044715 * cube)))) * up
        act[pl.ds(2 * e, 2)] = activated.reshape(2, 128, 384)
        hidden = (activated * rescale[...].reshape(1, 384)).astype(bf16)
        total = jnp.dot(hidden, w_out[...], preferred_element_type=f32)
        total = total.reshape(2, 2, 4, 16, 1024)
        part[pl.ds(2 * e, 2)] = total
        out1[pl.ds(2 * e, 2)] = coded(total)

    loads[0].wait()
    loads[1].wait()
    first.own()
    feed_forward(y)
    first.r4()
    first.r5()
    first.minus()
    feed_forward(ym)
    first.plus()
    feed_forward(yp)
    first.far()
    feed_forward(yo)

    sums = [
        Sum(place, g, part, out1, halves1, quarters1, s_send.at[g], s_recv.at[g], log)
        for g in range(2)
    ]
    for s in sums:
        s.s0_far()
    for s in sums:
        s.s0_plus()
        s.s0_minus()
    for s in sums:
        s.s0_own()
    for s in sums:
        s.s1()
    for s in sums:
        s.s2()
    for s in sums:
        s.s3()

    def gather_of(ref, sends, recvs, g):
        return Gather(
            place,
            lambda y, z, part: ref.at[g * 4 + y, z, pl.ds(*part)],
            sends.at[g],
            recvs.at[g],
            log,
        )

    nexts = [gather_of(normed, g2_send.at[0], g2_recv.at[0], g) for g in range(2)]
    lasts = [gather_of(grads, g2_send.at[1], g2_recv.at[1], g) for g in range(2)]

    def normed_rows(g):
        inputs = x[g * 4 + y, pl.ds(2 * z, 2)].reshape(64, 1024).astype(f32)
        residual = inputs + sums[g].result()
        res[g] = residual
        inverse = lax.rsqrt(jnp.mean(residual * residual, axis=-1, keepdims=True) + epsilon)
        n = (residual * inverse * final_gain[...]).astype(bf16)
        normed[g * 4 + y, z] = n.reshape(4, 16, 1024)

    lane = lax.broadcasted_iota(jnp.int32, (128, 128), 1)

    def wanted_of(b):
        return tgt[b] - (place * 2048).astype(f32) - lane.astype(f32)

    def logit_block(g, yy):
        b = g * 4 + yy
        n = normed[b].reshape(128, 1024)
        wanted = wanted_of(b)
        state = [
            (
                jnp.full((HALF, 128), -jnp.inf, f32),
                jnp.zeros((HALF, 128), f32),
                jnp.zeros((HALF, 128), f32),
            )
            for _ in range(128 // HALF)
        ]

        def tally(j):
            for i, (top, total, hit) in enumerate(state):
                r = slice(i * HALF, (i + 1) * HALF)
                starts = [j * TILE + k * 128 for k in range(TILE // 128)]
                values = [logits[b, r, c : c + 128] for c in starts]
                new = top
                for value in values:
                    new = jnp.maximum(new, value)
                total = total * jnp.exp(top - new)
                for c, value in zip(starts, values):
                    total = total + jnp.exp(value - new)
                    hit = hit + jnp.where(wanted[r] == c, value, 0.0)
                state[i] = (new, total, hit)

        tiles = 2048 // TILE
        for j in range(tiles):
            c = j * TILE
            logits[b, :, c : c + TILE] = jnp.dot(
                n, w_head[:, c : c + TILE], preferred_element_type=f32
            )
            if j:
                tally(j - 1)
        tally(tiles - 1)
        lanes, total, hit = (jnp.concatenate(v, axis=0) for v in zip(*state))
        top = jnp.max(lanes, axis=1, keepdims=True)
        total = jnp.sum(total * jnp.exp(lanes - top), axis=1, keepdims=True)
        hit = jnp.sum(hit, axis=1, keepdims=True)
        table = jnp.where(lane == 0, top, jnp.where(lane == 1, total, hit))
        table = jnp.transpose(table)
        for k in range(3):
            stat[g, place, pl.ds(4 * k + yy, 1), :] = table[k : k + 1]

    def stat_copy(g, k):
        ref = stat.at[g, place]
        return pltpu.make_async_remote_copy(
            src_ref=ref,
            dst_ref=ref,
            send_sem=t_send.at[g, k - 1],
            recv_sem=t_recv.at[g, k - 1],
            device_id={"mp": (place + k) % 8},
            device_id_type=pl.DeviceIdType.MESH,
        )

    def send_stats(g):
        for k in range(1, 8):
            c = stat_copy(g, k)
            c.start()
            log.append(c)

    def wait_stats(g):
        for k in range(1, 8):
            ref = stat.at[g, (place + 8 - k) % 8]
            pltpu.make_async_remote_copy(
                src_ref=ref,
                dst_ref=ref,
                send_sem=t_send.at[g, k - 1],
                recv_sem=t_recv.at[g, k - 1],
                device_id={"mp": (place + k) % 8},
                device_id_type=pl.DeviceIdType.MESH,
            ).wait_recv()

    right = jnp.int32(0)
    whole = jnp.int32(0)
    for e in range(4):
        for c in range(4):
            right = right + jnp.where(labels[e] == c, lengths[e, c], 0)
            whole = whole + lengths[e, c]
    n_right = right.astype(f32)
    n_wrong = (whole - right).astype(f32)

    def loss_rows(g):
        top = stat[g, 0, 0:4]
        for k in range(1, 8):
            top = jnp.maximum(top, stat[g, k, 0:4])
        total = jnp.zeros((4, 128), f32)
        hit = jnp.zeros((4, 128), f32)
        for k in range(8):
            total = total + stat[g, k, 4:8] * jnp.exp(stat[g, k, 0:4] - top)
            hit = hit + stat[g, k, 8:12]
        log_norm = top + jnp.log(total)
        log_probs = hit - log_norm
        row = lax.broadcasted_iota(jnp.int32, (4, 128), 0)
        col = lax.broadcasted_iota(jnp.int32, (4, 128), 1)
        choice = (row % 2) * 2 + col // 64
        length = jnp.zeros((4, 128), jnp.int32)
        label = jnp.zeros((4, 128), jnp.int32)
        for i in range(4):
            e = g * 2 + i // 2
            label = jnp.where(row == i, labels[e], label)
            for s in range(2):
                here = (row == i) & (col // 64 == s)
                length = jnp.where(here, lengths[e, (i % 2) * 2 + s], length)
        valid = col % 64 < length
        correct = choice == label
        counts = length.astype(f32)
        kept = jnp.where(valid, log_probs, 0.0)
        low = jnp.sum(jnp.where(col < 64, kept, 0.0), axis=1, keepdims=True)
        high = jnp.sum(jnp.where(col < 64, 0.0, kept), axis=1, keepdims=True)
        average = jnp.where(col < 64, low, high) / counts
        safe = jnp.where(valid, log_probs, -1.0)
        prob = jnp.exp(safe)
        wrong = valid & ~correct
        terms = jnp.where(correct, kept, 0.0) / n_right
        terms = terms + jnp.where(wrong, jnp.log1p(-prob), 0.0) / n_wrong
        fines = []
        shares = []
        for i in range(2):
            a = average[2 * i : 2 * i + 2]
            shift = a - jnp.max(jnp.max(a, axis=1, keepdims=True), axis=0, keepdims=True)
            power = jnp.exp(shift)
            bulk = jnp.sum(jnp.sum(power, axis=1, keepdims=True), axis=0, keepdims=True)
            bulk = bulk * (1.0 / 64.0)
            shares.append(power / bulk)
            fines.append(shift - jnp.log(bulk))
        share = jnp.concatenate(shares, axis=0)
        weight = jnp.where(correct, -1.0 / n_right, prob / (1.0 - prob) / n_wrong)
        weight = weight - 0.25 * (jnp.where(correct, 1.0, 0.0) - share) / counts
        rows[g, 0:4] = log_norm
        rows[g, 4:8] = jnp.where(valid, weight, 0.0)
        fine = jnp.where(correct, jnp.concatenate(fines, axis=0), 0.0)
        return -terms - fine * (0.25 / 64.0)

    def columns(row):
        return jnp.transpose(jnp.broadcast_to(row, (128, 128)))

    def softer(g, yy, slot):
        b = g * 4 + yy
        norm = columns(rows[g, pl.ds(yy, 1), :])
        weight = columns(rows[g, pl.ds(4 + yy, 1), :])
        wanted = wanted_of(b)

        def step(j):
            for k in range(TILE // 128):
                c = j * TILE + k * 128
                soft = jnp.exp(logits[b, :, c : c + 128] - norm)
                hot = jnp.where(wanted == c, 1.0, 0.0)
                lgrad[slot, :, c : c + 128] = (weight * (hot - soft)).astype(bf16)

        return step

    def grad_blocks(g, order, sends):
        step = softer(g, order[0], 0)
        for j in range(4):
            step(j)
        for i, yy in enumerate(order):
            b = g * 4 + yy
            step = softer(g, order[i + 1], (i + 1) % 2) if i + 1 < len(order) else None
            for j in range(4):
                value = jnp.dot(
                    lgrad[i % 2], w_head_t[:, j * 256 : (j + 1) * 256], preferred_element_type=f32
                )
                part[b, :, :, :, j * 256 : (j + 1) * 256] = value.reshape(2, 4, 16, 256)
                if step is not None:
                    step(j)
            out2[b] = coded(part[b])
            sends[i]()

    normed_rows(0)
    nexts[0].s0()
    normed_rows(1)
    nexts[1].s0()
    nexts[0].r1()
    nexts[0].r2()
    nexts[1].r1()
    nexts[1].r2()
    nexts[0].r3()
    nexts[0].own()
    nexts[0].r4()
    nexts[0].r5()
    logit_block(0, y)
    nexts[1].r3()
    nexts[1].r4()
    nexts[0].minus()
    logit_block(0, ym)
    nexts[1].r5()
    nexts[0].plus()
    logit_block(0, yp)
    nexts[0].far()
    logit_block(0, yo)
    send_stats(0)
    nexts[1].own()
    logit_block(1, y)
    nexts[1].minus()
    logit_block(1, ym)
    nexts[1].plus()
    logit_block(1, yp)
    nexts[1].far()
    logit_block(1, yo)
    send_stats(1)
    wait_stats(0)
    loss = loss_rows(0)

    sums2 = [
        Sum(place, g, part, out2, halves2, quarters2, s_send.at[2 + g], s_recv.at[2 + g], log)
        for g in range(2)
    ]
    s = sums2[0]
    grad_blocks(0, (yo, yp, ym, y), (s.s0_far, s.s0_plus, s.s0_minus, s.s0_own))
    sums2[0].s1()
    sums2[0].s2()
    wait_stats(1)
    loss = loss + loss_rows(1)
    sums2[0].s3()
    s = sums2[1]
    grad_blocks(1, (yo, yp, ym, y), (s.s0_far, s.s0_plus, s.s0_minus, s.s0_own))

    def grad_rows(g):
        residual = res[g]
        inverse = lax.rsqrt(jnp.mean(residual * residual, axis=-1, keepdims=True) + epsilon)
        scaled = sums2[g].result() * final_gain[...]
        inner = jnp.mean(scaled * residual, axis=-1, keepdims=True)
        value = inverse * scaled - residual * (inverse * inverse * inverse) * inner
        grads[g * 4 + y, z] = value.astype(bf16).reshape(4, 16, 1024)

    def scale_block(g, yy):
        b = g * 4 + yy
        back = jnp.dot(grads[b].reshape(128, 1024), w_out_t[...], preferred_element_type=f32)
        acc[...] += jnp.sum((back * act[b]).reshape(16, 8, 384), axis=0)

    sent = len(log)
    grad_rows(0)
    lasts[0].s0()
    loss_out[0] = jnp.sum(loss)
    sums2[1].s1()
    sums2[1].s2()
    lasts[0].r1()
    lasts[0].r2()
    sums2[1].s3()
    lasts[0].r3()
    lasts[0].r4()
    lasts[0].r5()
    grad_rows(1)
    lasts[1].s0()
    for c in log[:sent]:
        c.wait_send()
    lasts[0].own()
    scale_block(0, y)
    lasts[1].r1()
    lasts[1].r2()
    lasts[0].minus()
    scale_block(0, ym)
    lasts[1].r3()
    lasts[0].plus()
    scale_block(0, yp)
    lasts[1].r4()
    lasts[1].r5()
    lasts[0].far()
    scale_block(0, yo)
    lasts[1].own()
    scale_block(1, y)
    lasts[1].minus()
    scale_block(1, ym)
    lasts[1].plus()
    scale_block(1, yp)
    lasts[1].far()
    scale_block(1, yo)
    scale_grad[...] = jnp.sum(acc[...], axis=0)
    for c in log[sent:]:
        c.wait_send()


def per_device(
    hidden_in, ff_gain, w_gate, w_up, w_out, ff_rescale, final_gain, w_head, targets, lengths, labels
):
    vmem = pl.BlockSpec(memory_space=pltpu.VMEM)
    smem = pl.BlockSpec(memory_space=pltpu.SMEM)
    hbm = pl.BlockSpec(memory_space=pl.ANY)
    dma = pltpu.SemaphoreType.DMA
    scale_grad, loss = pl.pallas_call(
        kernel,
        out_shape=(
            jax.ShapeDtypeStruct((384,), f32),
            jax.ShapeDtypeStruct((1,), f32),
        ),
        in_specs=[hbm] * 11,
        out_specs=(vmem, smem),
        scratch_shapes=[
            pltpu.VMEM((8, 4, 32, 1024), bf16),
            pltpu.VMEM((1024, 768), bf16),
            pltpu.VMEM((384, 1024), bf16),
            pltpu.VMEM((1024, 384), bf16),
            pltpu.VMEM((1024, 2048), bf16),
            pltpu.VMEM((2048, 1024), bf16),
            pltpu.VMEM((8, 128, 384), f32),
            pltpu.VMEM((8, 128, 128), f32),
            pltpu.VMEM((8, 2, 4, 16, 1024), f32),
            pltpu.VMEM((8, 2, 4, 16, WIDE), jnp.int16),
            pltpu.VMEM((8, 2, 4, 16, WIDE), jnp.int16),
            pltpu.VMEM((2, 11, 2, 16, WIDE), jnp.int16),
            pltpu.VMEM((2, 6, 1, 16, WIDE), jnp.int16),
            pltpu.VMEM((2, 11, 2, 16, WIDE), jnp.int16),
            pltpu.VMEM((2, 6, 1, 16, WIDE), jnp.int16),
            pltpu.VMEM((8, 2, 4, 16, 1024), bf16),
            pltpu.VMEM((8, 2, 4, 16, 1024), bf16),
            pltpu.VMEM((8, 128, 2048), f32),
            pltpu.VMEM((2, 128, 2048), bf16),
            pltpu.VMEM((2, 64, 1024), f32),
            pltpu.VMEM((2, 8, 16, 128), f32),
            pltpu.VMEM((2, 8, 128), f32),
            pltpu.VMEM((8, 384), f32),
            pltpu.VMEM((1, 1024), f32),
            pltpu.VMEM((1, 1024), f32),
            pltpu.VMEM((384,), f32),
            pltpu.VMEM((8, 128), jnp.int32),
            pltpu.SMEM((4, 4), jnp.int32),
            pltpu.SMEM((4,), jnp.int32),
            dma((11,)),
            dma((GATHER_MESSAGES,)),
            dma((GATHER_MESSAGES,)),
            dma((2, 2, GATHER_MESSAGES)),
            dma((2, 2, GATHER_MESSAGES)),
            dma((4, SUM_MESSAGES)),
            dma((4, SUM_MESSAGES)),
            dma((2, 7)),
            dma((2, 7)),
        ],
        compiler_params=pltpu.CompilerParams(
            collective_id=0, has_side_effects=True, vmem_limit_bytes=62 * 1024 * 1024
        ),
    )(
        hidden_in.reshape(4, 32, 1024),
        w_gate,
        w_up,
        w_out,
        w_head,
        ff_gain.reshape(1, 1024),
        final_gain.reshape(1, 1024),
        ff_rescale,
        targets.reshape(8, 128),
        lengths,
        labels,
    )
    return (scale_grad, loss)


def solution(mesh):
    return jax.shard_map(
        per_device,
        mesh=mesh,
        in_specs=(
            P(("task", "mp"), None),
            P(),
            P(None, "mp"),
            P(None, "mp"),
            P("mp", None),
            P(("task", "mp")),
            P(),
            P(None, "mp"),
            P("task"),
            P("task", None),
            P("task"),
        ),
        out_specs=(P(("task", "mp")), P("task")),
        check_vma=False,
    )
```

```python
import functools
import math

import jax
import jax.numpy as jnp
from jax import lax
from jax.experimental import pallas as pl
from jax.experimental.pallas import tpu as pltpu
from jax.sharding import PartitionSpec as P

f32 = jnp.float32
bf16 = jnp.bfloat16
epsilon = 1e-06
ROOT = math.sqrt(2.0 / math.pi)
TILE = 512
HALF = 64
STEPS = 256.0
TOP = 32700.0
WIDE = 1024 + 128

A, B = (0, 2), (2, 2)
AP, AM, BP, BM = (0, 1), (1, 1), (2, 1), (3, 1)


def coded(total):
    top = jnp.max(jnp.abs(total), axis=-1, keepdims=True)
    top = jnp.broadcast_to(jnp.maximum(top, 1e-30), (*total.shape[:-1], 128))
    power = jnp.ceil(jnp.log(top) * (STEPS / math.log(2.0)))
    factor = TOP * jnp.exp(power * (-math.log(2.0) / STEPS))
    value = jnp.round(total * jnp.concatenate([factor] * 8, axis=-1))
    both = jnp.concatenate([value, power], axis=-1)
    return both.astype(jnp.int32).astype(jnp.int16)


def decoded(code):
    both = code.astype(jnp.int32).astype(f32)
    factor = jnp.exp(both[..., 1024:] * (math.log(2.0) / STEPS)) * (1.0 / TOP)
    return both[..., :1024] * jnp.concatenate([factor] * 8, axis=-1)


class Links:
    def __init__(self, place, sends, recvs, log):
        y, z = place // 2, place % 2
        self.y, self.z = y, z
        self.yp, self.ym, self.yo = (y + 1) % 4, (y + 3) % 4, (y + 2) % 4
        self.oz = 1 - z
        self.to = {"z": y * 2 + (1 - z), "p": self.yp * 2 + z, "m": self.ym * 2 + z}
        self.sends, self.recvs, self.log = sends, recvs, log

    def copy(self, k, src, dst, way):
        return pltpu.make_async_remote_copy(
            src_ref=src,
            dst_ref=dst,
            send_sem=self.sends.at[k],
            recv_sem=self.recvs.at[k],
            device_id={"mp": self.to[way]},
            device_id_type=pl.DeviceIdType.MESH,
        )

    def send(self, k, src, dst, way):
        c = self.copy(k, src, dst, way)
        c.start()
        self.log.append(c)

    def got(self, k, dst):
        self.copy(k, dst, dst, "z").wait_recv()


class Gather(Links):
    def __init__(self, place, at, sends, recvs, log):
        super().__init__(place, sends, recvs, log)
        self.at = at

    def put(self, k, y, z, part, way):
        ref = self.at(y, z, part)
        self.send(k, ref, ref, way)

    def have(self, k, y, z, part):
        self.got(k, self.at(y, z, part))

    def s0(self):
        y, z = self.y, self.z
        self.put(0, y, z, A, "z")
        self.put(2, y, z, B, "p")
        self.put(3, y, z, B, "m")
        self.put(1, y, z, B, "z")
        self.put(4, y, z, A, "p")
        self.put(5, y, z, A, "m")

    def r1(self):
        self.have(2, self.ym, self.z, B)
        self.put(6, self.ym, self.z, BP, "p")
        self.put(15, self.ym, self.z, B, "z")
        self.have(3, self.yp, self.z, B)
        self.put(7, self.yp, self.z, BM, "m")
        self.put(14, self.yp, self.z, B, "z")

    def r2(self):
        self.have(0, self.y, self.oz, A)
        self.put(8, self.y, self.oz, A, "p")
        self.put(9, self.y, self.oz, A, "m")

    def r3(self):
        self.have(4, self.ym, self.z, A)
        self.put(10, self.ym, self.z, AP, "p")
        self.have(5, self.yp, self.z, A)
        self.put(11, self.yp, self.z, AM, "m")

    def r4(self):
        self.have(6, self.yo, self.z, BP)
        self.put(16, self.yo, self.z, BP, "z")
        self.have(7, self.yo, self.z, BM)
        self.put(17, self.yo, self.z, BM, "z")

    def r5(self):
        self.have(8, self.ym, self.oz, A)
        self.put(12, self.ym, self.oz, AP, "p")
        self.have(9, self.yp, self.oz, A)
        self.put(13, self.yp, self.oz, AM, "m")

    def own(self):
        self.have(1, self.y, self.oz, B)

    def plus(self):
        self.have(14, self.yp, self.oz, B)

    def minus(self):
        self.have(15, self.ym, self.oz, B)

    def far(self):
        self.far_near()
        self.far_across()

    def far_near(self):
        self.have(10, self.yo, self.z, AP)
        self.have(11, self.yo, self.z, AM)

    def far_across(self):
        self.have(12, self.yo, self.oz, AP)
        self.have(13, self.yo, self.oz, AM)
        self.have(16, self.yo, self.oz, BP)
        self.have(17, self.yo, self.oz, BM)


class Sum(Links):
    def __init__(self, place, g, part, out, halves, quarters, sends, recvs, log):
        super().__init__(place, sends, recvs, log)
        self.g, self.part, self.out, self.halves, self.quarters = g, part, out, halves, quarters

    def at(self, ref, y, z, part):
        return ref.at[self.g * 4 + y, z, pl.ds(*part)]

    def h(self, k):
        return self.halves.at[self.g, k]

    def q(self, k):
        return self.quarters.at[self.g, k]

    def s0_far_y(self):
        yo = self.yo
        for z in range(2):
            self.send(4 + 9 * z, self.at(self.out, yo, z, AP), self.q(0 + z), "p")
            self.send(5 + 9 * z, self.at(self.out, yo, z, AM), self.q(2 + z), "m")

    def s0_far_z(self):
        self.send(0, self.at(self.out, self.yo, self.oz, B), self.h(0), "z")

    def s0_far(self):
        self.s0_far_y()
        self.s0_far_z()

    def s0_plus(self):
        self.send(1, self.at(self.out, self.yp, self.oz, B), self.h(1), "z")

    def s0_minus(self):
        self.send(2, self.at(self.out, self.ym, self.oz, B), self.h(2), "z")

    def s0_own(self):
        self.send(3, self.at(self.out, self.y, self.oz, B), self.h(3), "z")

    def add(self, y, z, part, *refs):
        total = self.at(self.part, y, z, part)[...]
        for ref in refs:
            total = total + decoded(ref[...])
        self.at(self.out, y, z, part)[...] = coded(total)

    def s1b(self):
        self.got(0, self.h(0))
        self.add(self.yo, self.z, B, self.h(0))
        self.send(8, self.at(self.out, self.yo, self.z, BP), self.q(4), "p")
        self.send(9, self.at(self.out, self.yo, self.z, BM), self.q(5), "m")

    def s1(self):
        self.s1b()
        self.s1a()

    def s1a(self):
        for z in range(2):
            self.got(4 + 9 * z, self.q(0 + z))
            self.add(self.yp, z, AP, self.q(0 + z))
            self.send(6 + 9 * z, self.at(self.out, self.yp, z, A), self.h(4 + z), "p")
            self.got(5 + 9 * z, self.q(2 + z))
            self.add(self.ym, z, AM, self.q(2 + z))
            self.send(7 + 9 * z, self.at(self.out, self.ym, z, A), self.h(6 + z), "m")

    def s2(self):
        self.got(1, self.h(1))
        self.got(8, self.q(4))
        h = self.h(1)
        self.add(self.yp, self.z, BP, h.at[pl.ds(0, 1)], self.q(4))
        self.add(self.yp, self.z, BM, h.at[pl.ds(1, 1)])
        self.send(10, self.at(self.out, self.yp, self.z, B), self.h(8), "p")
        self.got(2, self.h(2))
        self.got(9, self.q(5))
        h = self.h(2)
        self.add(self.ym, self.z, BP, h.at[pl.ds(0, 1)])
        self.add(self.ym, self.z, BM, h.at[pl.ds(1, 1)], self.q(5))
        self.send(11, self.at(self.out, self.ym, self.z, B), self.h(9), "m")

    def s3(self):
        for z in range(2):
            self.got(6 + 9 * z, self.h(4 + z))
            self.got(7 + 9 * z, self.h(6 + z))
        self.add(self.y, self.oz, A, self.h(4 + self.oz), self.h(6 + self.oz))
        self.send(12, self.at(self.out, self.y, self.oz, A), self.h(10), "z")

    def result(self):
        self.got(3, self.h(3))
        self.got(10, self.h(8))
        self.got(11, self.h(9))
        self.got(12, self.h(10))
        halves = []
        for part, slots in ((A, (4 + self.z, 6 + self.z, 10)), (B, (3, 8, 9))):
            total = self.at(self.part, self.y, self.z, part)[...]
            for k in slots:
                total = total + decoded(self.h(k)[...])
            halves.append(total.reshape(32, 1024))
        return jnp.concatenate(halves, axis=0)


SUM_MESSAGES = 17
GATHER_MESSAGES = 18


def kernel(
    hidden_hbm,
    gate_hbm,
    up_hbm,
    out_hbm,
    head_hbm,
    ff_gain_hbm,
    final_gain_hbm,
    rescale_hbm,
    targets_hbm,
    lengths_hbm,
    labels_hbm,
    scale_grad,
    loss_out,
    x,
    w_in,
    w_out,
    w_out_t,
    w_head,
    w_head_t,
    act,
    tgt,
    part,
    out1,
    out2,
    halves1,
    quarters1,
    halves2,
    quarters2,
    normed,
    grads,
    logits,
    lgrad,
    res,
    stat,
    rows,
    acc,
    ff_gain,
    final_gain,
    rescale,
    targets,
    lengths,
    labels,
    local_sem,
    g1_send,
    g1_recv,
    g2_send,
    g2_recv,
    s_send,
    s_recv,
    t_send,
    t_recv,
):
    place = lax.axis_index("mp")
    log = []
    own = pltpu.make_async_copy(hidden_hbm, x.at[place], local_sem.at[0])
    loads = [
        pltpu.make_async_copy(gate_hbm, w_in.at[:, pl.ds(0, 384)], local_sem.at[1]),
        pltpu.make_async_copy(up_hbm, w_in.at[:, pl.ds(384, 384)], local_sem.at[2]),
        pltpu.make_async_copy(out_hbm, w_out, local_sem.at[3]),
        pltpu.make_async_copy(head_hbm, w_head, local_sem.at[4]),
    ]
    small = [
        pltpu.make_async_copy(src, dst, local_sem.at[5 + k])
        for k, (src, dst) in enumerate(
            (
                (targets_hbm, targets),
                (ff_gain_hbm, ff_gain),
                (rescale_hbm, rescale),
                (final_gain_hbm, final_gain),
                (lengths_hbm, lengths),
                (labels_hbm, labels),
            )
        )
    ]
    own.start()
    for c in (*small, *loads):
        c.start()

    barrier = pltpu.get_barrier_semaphore()
    for k in range(1, 8):
        pl.semaphore_signal(
            barrier,
            inc=1,
            device_id={"mp": (place + k) % 8},
            device_id_type=pl.DeviceIdType.MESH,
        )
    pl.semaphore_wait(barrier, 7)
    own.wait()

    first = Gather(
        place, lambda y, z, part: x.at[y * 2 + z, pl.ds(*part)], g1_send, g1_recv, log
    )
    first.s0()
    y, z, yp, ym, yo = first.y, first.z, first.yp, first.ym, first.yo

    def target_block(i, _):
        row = targets[pl.ds(i, 1), :].astype(f32)
        tgt[i] = jnp.transpose(jnp.broadcast_to(row, (128, 128)))
        return 0

    def head_block(i, _):
        r = pl.multiple_of((i // 8) * 256, 256)
        c = pl.multiple_of((i % 8) * 256, 256)
        w_head_t[pl.ds(c, 256), pl.ds(r, 256)] = jnp.transpose(
            w_head[pl.ds(r, 256), pl.ds(c, 256)]
        )
        return 0

    def out_block(i, _):
        r = pl.multiple_of((i // 4) * 128, 128)
        c = pl.multiple_of((i % 4) * 256, 256)
        w_out_t[pl.ds(c, 256), pl.ds(r, 128)] = jnp.transpose(
            w_out[pl.ds(r, 128), pl.ds(c, 256)]
        )
        return 0

    for c in small:
        c.wait()
    lax.fori_loop(0, 8, target_block, 0)
    acc[...] = jnp.zeros_like(acc)
    stat[...] = jnp.zeros_like(stat)
    loads[2].wait()
    lax.fori_loop(0, 12, out_block, 0)
    loads[3].wait()
    first.r1()
    first.r2()
    lax.fori_loop(0, 32, head_block, 0)
    first.r3()

    def feed_forward(first_chunk, count):
        here = pl.ds(first_chunk, count)
        rows2 = x[here].reshape(count * 128, 1024).astype(f32)
        inverse = lax.rsqrt(jnp.mean(rows2 * rows2, axis=-1, keepdims=True) + epsilon)
        n = (rows2 * inverse * ff_gain[...]).astype(bf16)
        both = jnp.dot(n, w_in[...], preferred_element_type=f32)
        gate, up = both[:, :384], both[:, 384:]
        cube = gate * gate * gate
        activated = gate * (0.5 * (1.0 + jnp.tanh(ROOT * (gate + 0.044715 * cube)))) * up
        act[here] = activated.reshape(count, 128, 384)
        hidden = (activated * rescale[...].reshape(1, 384)).astype(bf16)
        total = jnp.dot(hidden, w_out[...], preferred_element_type=f32)
        total = total.reshape(count, 2, 4, 16, 1024)
        part[here] = total
        out1[here] = coded(total)

    loads[0].wait()
    loads[1].wait()
    first.own()
    feed_forward(2 * y, 2)
    first.r4()
    first.r5()
    first.minus()
    feed_forward(2 * ym, 2)
    first.plus()
    feed_forward(2 * yp, 2)
    first.far_near()
    feed_forward(2 * yo + z, 1)
    first.far_across()
    feed_forward(2 * yo + 1 - z, 1)

    sums = [
        Sum(place, g, part, out1, halves1, quarters1, s_send.at[g], s_recv.at[g], log)
        for g in range(2)
    ]
    for s in sums:
        s.s0_far()
    for s in sums:
        s.s0_plus()
        s.s0_minus()
    for s in sums:
        s.s0_own()
    for s in sums:
        s.s1()
    for s in sums:
        s.s2()
    for s in sums:
        s.s3()

    def gather_of(ref, sends, recvs, g):
        return Gather(
            place,
            lambda y, z, part: ref.at[g * 4 + y, z, pl.ds(*part)],
            sends.at[g],
            recvs.at[g],
            log,
        )

    nexts = [gather_of(normed, g2_send.at[0], g2_recv.at[0], g) for g in range(2)]
    lasts = [gather_of(grads, g2_send.at[1], g2_recv.at[1], g) for g in range(2)]

    def normed_rows(g):
        inputs = x[g * 4 + y, pl.ds(2 * z, 2)].reshape(64, 1024).astype(f32)
        residual = inputs + sums[g].result()
        res[g] = residual
        inverse = lax.rsqrt(jnp.mean(residual * residual, axis=-1, keepdims=True) + epsilon)
        n = (residual * inverse * final_gain[...]).astype(bf16)
        normed[g * 4 + y, z] = n.reshape(4, 16, 1024)

    lane = lax.broadcasted_iota(jnp.int32, (128, 128), 1)

    def wanted_of(b):
        return tgt[b] - (place * 2048).astype(f32) - lane.astype(f32)

    def logit_block(g, yy):
        b = g * 4 + yy
        n = normed[b].reshape(128, 1024)
        wanted = wanted_of(b)
        state = [
            (
                jnp.full((HALF, 128), -jnp.inf, f32),
                jnp.zeros((HALF, 128), f32),
                jnp.zeros((HALF, 128), f32),
            )
            for _ in range(128 // HALF)
        ]

        def tally(j):
            for i, (top, total, hit) in enumerate(state):
                r = slice(i * HALF, (i + 1) * HALF)
                starts = [j * TILE + k * 128 for k in range(TILE // 128)]
                values = [logits[b, r, c : c + 128] for c in starts]
                new = top
                for value in values:
                    new = jnp.maximum(new, value)
                total = total * jnp.exp(top - new)
                for c, value in zip(starts, values):
                    total = total + jnp.exp(value - new)
                    hit = hit + jnp.where(wanted[r] == c, value, 0.0)
                state[i] = (new, total, hit)

        tiles = 2048 // TILE
        for j in range(tiles):
            c = j * TILE
            logits[b, :, c : c + TILE] = jnp.dot(
                n, w_head[:, c : c + TILE], preferred_element_type=f32
            )
            if j:
                tally(j - 1)
        tally(tiles - 1)
        lanes, total, hit = (jnp.concatenate(v, axis=0) for v in zip(*state))
        top = jnp.max(lanes, axis=1, keepdims=True)
        total = jnp.sum(total * jnp.exp(lanes - top), axis=1, keepdims=True)
        hit = jnp.sum(hit, axis=1, keepdims=True)
        table = jnp.where(lane == 0, top, jnp.where(lane == 1, total, hit))
        table = jnp.transpose(table)
        for k in range(3):
            stat[g, place, pl.ds(4 * k + yy, 1), :] = table[k : k + 1]

    def stat_copy(g, k):
        ref = stat.at[g, place]
        return pltpu.make_async_remote_copy(
            src_ref=ref,
            dst_ref=ref,
            send_sem=t_send.at[g, k - 1],
            recv_sem=t_recv.at[g, k - 1],
            device_id={"mp": (place + k) % 8},
            device_id_type=pl.DeviceIdType.MESH,
        )

    def send_stats(g):
        for k in range(1, 8):
            c = stat_copy(g, k)
            c.start()
            log.append(c)

    def wait_stats(g):
        for k in range(1, 8):
            ref = stat.at[g, (place + 8 - k) % 8]
            pltpu.make_async_remote_copy(
                src_ref=ref,
                dst_ref=ref,
                send_sem=t_send.at[g, k - 1],
                recv_sem=t_recv.at[g, k - 1],
                device_id={"mp": (place + k) % 8},
                device_id_type=pl.DeviceIdType.MESH,
            ).wait_recv()

    right = jnp.int32(0)
    whole = jnp.int32(0)
    for e in range(4):
        for c in range(4):
            right = right + jnp.where(labels[e] == c, lengths[e, c], 0)
            whole = whole + lengths[e, c]
    n_right = right.astype(f32)
    n_wrong = (whole - right).astype(f32)

    def loss_rows(g):
        top = stat[g, 0, 0:4]
        for k in range(1, 8):
            top = jnp.maximum(top, stat[g, k, 0:4])
        total = jnp.zeros((4, 128), f32)
        hit = jnp.zeros((4, 128), f32)
        for k in range(8):
            total = total + stat[g, k, 4:8] * jnp.exp(stat[g, k, 0:4] - top)
            hit = hit + stat[g, k, 8:12]
        log_norm = top + jnp.log(total)
        log_probs = hit - log_norm
        row = lax.broadcasted_iota(jnp.int32, (4, 128), 0)
        col = lax.broadcasted_iota(jnp.int32, (4, 128), 1)
        choice = (row % 2) * 2 + col // 64
        length = jnp.zeros((4, 128), jnp.int32)
        label = jnp.zeros((4, 128), jnp.int32)
        for i in range(4):
            e = g * 2 + i // 2
            label = jnp.where(row == i, labels[e], label)
            for s in range(2):
                here = (row == i) & (col // 64 == s)
                length = jnp.where(here, lengths[e, (i % 2) * 2 + s], length)
        valid = col % 64 < length
        correct = choice == label
        counts = length.astype(f32)
        kept = jnp.where(valid, log_probs, 0.0)
        low = jnp.sum(jnp.where(col < 64, kept, 0.0), axis=1, keepdims=True)
        high = jnp.sum(jnp.where(col < 64, 0.0, kept), axis=1, keepdims=True)
        average = jnp.where(col < 64, low, high) / counts
        safe = jnp.where(valid, log_probs, -1.0)
        prob = jnp.exp(safe)
        wrong = valid & ~correct
        terms = jnp.where(correct, kept, 0.0) / n_right
        terms = terms + jnp.where(wrong, jnp.log1p(-prob), 0.0) / n_wrong
        fines = []
        shares = []
        for i in range(2):
            a = average[2 * i : 2 * i + 2]
            shift = a - jnp.max(jnp.max(a, axis=1, keepdims=True), axis=0, keepdims=True)
            power = jnp.exp(shift)
            bulk = jnp.sum(jnp.sum(power, axis=1, keepdims=True), axis=0, keepdims=True)
            bulk = bulk * (1.0 / 64.0)
            shares.append(power / bulk)
            fines.append(shift - jnp.log(bulk))
        share = jnp.concatenate(shares, axis=0)
        weight = jnp.where(correct, -1.0 / n_right, prob / (1.0 - prob) / n_wrong)
        weight = weight - 0.25 * (jnp.where(correct, 1.0, 0.0) - share) / counts
        rows[g, 0:4] = log_norm
        rows[g, 4:8] = jnp.where(valid, weight, 0.0)
        fine = jnp.where(correct, jnp.concatenate(fines, axis=0), 0.0)
        return -terms - fine * (0.25 / 64.0)

    def columns(row):
        return jnp.transpose(jnp.broadcast_to(row, (128, 128)))

    def softer(g, yy, slot):
        b = g * 4 + yy
        norm = columns(rows[g, pl.ds(yy, 1), :])
        weight = columns(rows[g, pl.ds(4 + yy, 1), :])
        wanted = wanted_of(b)

        def step(j):
            for k in range(TILE // 128):
                c = j * TILE + k * 128
                soft = jnp.exp(logits[b, :, c : c + 128] - norm)
                hot = jnp.where(wanted == c, 1.0, 0.0)
                lgrad[slot, :, c : c + 128] = (weight * (hot - soft)).astype(bf16)

        return step

    def grad_blocks(g, order, sends):
        step = softer(g, order[0], 0)
        for j in range(4):
            step(j)
        for i, yy in enumerate(order):
            b = g * 4 + yy
            step = softer(g, order[i + 1], (i + 1) % 2) if i + 1 < len(order) else None
            for j in range(4):
                value = jnp.dot(
                    lgrad[i % 2], w_head_t[:, j * 256 : (j + 1) * 256], preferred_element_type=f32
                )
                part[b, :, :, :, j * 256 : (j + 1) * 256] = value.reshape(2, 4, 16, 256)
                if step is not None:
                    step(j)
            out2[b] = coded(part[b])
            sends[i]()

    normed_rows(0)
    nexts[0].s0()
    normed_rows(1)
    nexts[1].s0()
    nexts[0].r1()
    nexts[0].r2()
    nexts[1].r1()
    nexts[1].r2()
    nexts[0].r3()
    nexts[0].own()
    nexts[0].r4()
    nexts[0].r5()
    logit_block(0, y)
    nexts[1].r3()
    nexts[1].r4()
    nexts[0].minus()
    logit_block(0, ym)
    nexts[1].r5()
    nexts[0].plus()
    logit_block(0, yp)
    nexts[0].far()
    logit_block(0, yo)
    send_stats(0)
    nexts[1].own()
    logit_block(1, y)
    nexts[1].minus()
    logit_block(1, ym)
    nexts[1].plus()
    logit_block(1, yp)
    nexts[1].far()
    logit_block(1, yo)
    send_stats(1)
    wait_stats(0)
    loss = loss_rows(0)

    sums2 = [
        Sum(place, g, part, out2, halves2, quarters2, s_send.at[2 + g], s_recv.at[2 + g], log)
        for g in range(2)
    ]
    s = sums2[0]
    grad_blocks(0, (yo, yp, ym, y), (s.s0_far, s.s0_plus, s.s0_minus, s.s0_own))
    sums2[0].s1()
    sums2[0].s2()
    wait_stats(1)
    loss = loss + loss_rows(1)
    sums2[0].s3()
    s = sums2[1]
    grad_blocks(1, (yo, yp, ym, y), (s.s0_far, s.s0_plus, s.s0_minus, s.s0_own))

    def grad_rows(g):
        residual = res[g]
        inverse = lax.rsqrt(jnp.mean(residual * residual, axis=-1, keepdims=True) + epsilon)
        scaled = sums2[g].result() * final_gain[...]
        inner = jnp.mean(scaled * residual, axis=-1, keepdims=True)
        value = inverse * scaled - residual * (inverse * inverse * inverse) * inner
        grads[g * 4 + y, z] = value.astype(bf16).reshape(4, 16, 1024)

    def scale_block(g, yy):
        b = g * 4 + yy
        back = jnp.dot(grads[b].reshape(128, 1024), w_out_t[...], preferred_element_type=f32)
        acc[...] += jnp.sum((back * act[b]).reshape(16, 8, 384), axis=0)

    sent = len(log)
    grad_rows(0)
    lasts[0].s0()
    loss_out[0] = jnp.sum(loss)
    sums2[1].s1()
    sums2[1].s2()
    lasts[0].r1()
    lasts[0].r2()
    sums2[1].s3()
    lasts[0].r3()
    lasts[0].r4()
    lasts[0].r5()
    grad_rows(1)
    lasts[1].s0()
    for c in log[:sent]:
        c.wait_send()
    lasts[0].own()
    scale_block(0, y)
    lasts[1].r1()
    lasts[1].r2()
    lasts[0].minus()
    scale_block(0, ym)
    lasts[1].r3()
    lasts[0].plus()
    scale_block(0, yp)
    lasts[1].r4()
    lasts[1].r5()
    lasts[0].far()
    scale_block(0, yo)
    lasts[1].own()
    scale_block(1, y)
    lasts[1].minus()
    scale_block(1, ym)
    lasts[1].plus()
    scale_block(1, yp)
    lasts[1].far()
    scale_block(1, yo)
    scale_grad[...] = jnp.sum(acc[...], axis=0)
    for c in log[sent:]:
        c.wait_send()


def per_device(
    hidden_in, ff_gain, w_gate, w_up, w_out, ff_rescale, final_gain, w_head, targets, lengths, labels
):
    vmem = pl.BlockSpec(memory_space=pltpu.VMEM)
    smem = pl.BlockSpec(memory_space=pltpu.SMEM)
    hbm = pl.BlockSpec(memory_space=pl.ANY)
    dma = pltpu.SemaphoreType.DMA
    scale_grad, loss = pl.pallas_call(
        kernel,
        out_shape=(
            jax.ShapeDtypeStruct((384,), f32),
            jax.ShapeDtypeStruct((1,), f32),
        ),
        in_specs=[hbm] * 11,
        out_specs=(vmem, smem),
        scratch_shapes=[
            pltpu.VMEM((8, 4, 32, 1024), bf16),
            pltpu.VMEM((1024, 768), bf16),
            pltpu.VMEM((384, 1024), bf16),
            pltpu.VMEM((1024, 384), bf16),
            pltpu.VMEM((1024, 2048), bf16),
            pltpu.VMEM((2048, 1024), bf16),
            pltpu.VMEM((8, 128, 384), f32),
            pltpu.VMEM((8, 128, 128), f32),
            pltpu.VMEM((8, 2, 4, 16, 1024), f32),
            pltpu.VMEM((8, 2, 4, 16, WIDE), jnp.int16),
            pltpu.VMEM((8, 2, 4, 16, WIDE), jnp.int16),
            pltpu.VMEM((2, 11, 2, 16, WIDE), jnp.int16),
            pltpu.VMEM((2, 6, 1, 16, WIDE), jnp.int16),
            pltpu.VMEM((2, 11, 2, 16, WIDE), jnp.int16),
            pltpu.VMEM((2, 6, 1, 16, WIDE), jnp.int16),
            pltpu.VMEM((8, 2, 4, 16, 1024), bf16),
            pltpu.VMEM((8, 2, 4, 16, 1024), bf16),
            pltpu.VMEM((8, 128, 2048), f32),
            pltpu.VMEM((2, 128, 2048), bf16),
            pltpu.VMEM((2, 64, 1024), f32),
            pltpu.VMEM((2, 8, 16, 128), f32),
            pltpu.VMEM((2, 8, 128), f32),
            pltpu.VMEM((8, 384), f32),
            pltpu.VMEM((1, 1024), f32),
            pltpu.VMEM((1, 1024), f32),
            pltpu.VMEM((384,), f32),
            pltpu.VMEM((8, 128), jnp.int32),
            pltpu.SMEM((4, 4), jnp.int32),
            pltpu.SMEM((4,), jnp.int32),
            dma((11,)),
            dma((GATHER_MESSAGES,)),
            dma((GATHER_MESSAGES,)),
            dma((2, 2, GATHER_MESSAGES)),
            dma((2, 2, GATHER_MESSAGES)),
            dma((4, SUM_MESSAGES)),
            dma((4, SUM_MESSAGES)),
            dma((2, 7)),
            dma((2, 7)),
        ],
        compiler_params=pltpu.CompilerParams(
            collective_id=0, has_side_effects=True, vmem_limit_bytes=62 * 1024 * 1024
        ),
    )(
        hidden_in.reshape(4, 32, 1024),
        w_gate,
        w_up,
        w_out,
        w_head,
        ff_gain.reshape(1, 1024),
        final_gain.reshape(1, 1024),
        ff_rescale,
        targets.reshape(8, 128),
        lengths,
        labels,
    )
    return (scale_grad, loss)


def solution(mesh):
    return jax.shard_map(
        per_device,
        mesh=mesh,
        in_specs=(
            P(("task", "mp"), None),
            P(),
            P(None, "mp"),
            P(None, "mp"),
            P("mp", None),
            P(("task", "mp")),
            P(),
            P(None, "mp"),
            P("task"),
            P("task", None),
            P("task"),
        ),
        out_specs=(P(("task", "mp")), P("task")),
        check_vma=False,
    )
```
